32 devices in a mesh: dp: 1 (over z), dcp: 32 (over y, x, core).
Axes of the slice: x: 4, y: 4, z: 1, core: 2. Of those that a mesh axis runs over, the one named last changes fastest.
The devices are a block of a 4x4x8 slice.
Arguments:
- q: bfloat16 [64, 128, 576], P('dp', 'dcp')
- cache: bfloat16 [64, 64, 32, 8, 576], P('dp', None, 'dcp')
- lens: int32 [64], P('dp')
Outputs:
- output: bfloat16 [64, 128, 512], P('dp', 'dcp')
All inputs are finite; a program needn't handle non-finite values.
Results may differ from the reference program's by a relative error of at most 0.00773808.
Values are sent between devices in bfloat16 or wider.
A program may use at most 768 MiB of HBM per device.

```python
import jax
import jax.numpy as jnp
from jax import lax

B = 64
S = 16384
PAGE = 8
DCP = 32
HEADS = 128
LORA = 512
ROPE = 64
NOPE = 128

R = S // (PAGE * DCP)
K = LORA + ROPE


def setup_inputs(seed: int = 0, part: int = 0) -> dict:
    key = jax.random.fold_in(jax.random.key(seed), part)
    kq, kc, kl = jax.random.split(key, 3)
    qs = 1.5 * ((NOPE + ROPE) / 2.0) ** 0.5
    scale = jnp.concatenate([jnp.full((LORA,), qs / LORA ** 0.5, jnp.float32), jnp.full((ROPE,), qs / ROPE ** 0.5, jnp.float32)])
    q = (jax.random.normal(kq, (B, HEADS, K), jnp.float32) * scale).astype(jnp.bfloat16)
    cache = jax.random.normal(kc, (B, R, DCP, PAGE, K), jnp.float32).astype(jnp.bfloat16)
    lens = jax.random.randint(kl, (B,), S // 4, S + 1, jnp.int32)
    return {'q': q, 'cache': cache, 'lens': lens}


def reference(q, cache, lens):
    c = cache.reshape(B, S, K)
    pos = jnp.arange(S)

    def one(args):
        qb, cb, lb = args
        s = jnp.dot(qb, cb.T, preferred_element_type=jnp.float32) / (NOPE + ROPE) ** 0.5
        s = jnp.where(pos[None, :] < lb, s, -jnp.inf)
        a = jax.nn.softmax(s, axis=1)
        o = jnp.dot(a, cb[:, :LORA].astype(jnp.float32), preferred_element_type=jnp.float32)
        return o.astype(jnp.bfloat16)

    return lax.map(one, (q, c, lens))
```

```python
import functools
import math

import jax
import jax.numpy as jnp
from jax import lax
from jax.experimental import pallas as pl
from jax.experimental.pallas import tpu as pltpu
from jax.sharding import PartitionSpec as P

ROPE = 64
QK_DIM = 192
SCALE = QK_DIM ** -0.5
NEG = float('-inf')
LANES = 128
NBUF = 4


def kernel(n, side, nc, nb, page, q_ref, cache_ref, lens_ref, out_ref,
           g1, qall, cbuf, own, osend, orecv, p1s, p1r, l1s, l1r, p2s, p2r, l2s, l2r, wrow,
           csem, a1s, a1r, a2s, a2r, a3s, a3r, ods, odr, s1, r1, sl1, rl1, s2, r2, sl2, rl2):
    hl = q_ref.shape[1]
    k = q_ref.shape[2]
    t = cbuf.shape[1]
    lorav = k - ROPE
    tile = side * hl
    half = side * tile
    total = nc * nb

    me = lax.axis_index('dcp')
    core = me % 2
    x = (me // 2) % side
    y = me // (2 * side)
    dists = tuple(range(1, side))

    def at(yy, xx, cc):
        return {'dcp': (yy * side + xx) * 2 + cc}

    sib = at(y, x, 1 - core)

    def axes(c):
        ax = (x, lambda d: at(y, (x + d) % side, core))
        ay = (y, lambda d: at((y + d) % side, x, core))
        return (ax, ay) if c % 2 == 0 else (ay, ax)

    def rcopy(src, dst, ss, rs, dev):
        return pltpu.make_async_remote_copy(src_ref=src, dst_ref=dst, send_sem=ss, recv_sem=rs, device_id=dev,
                                            device_id_type=pl.DeviceIdType.MESH)

    def ag1(c, d):
        (m1, peer), _ = axes(c)
        return rcopy(q_ref.at[pl.ds(c * nb, nb)], g1.at[c, m1], a1s.at[c, d - 1], a1r.at[c, d - 1], peer(d))

    def ag2(c, d):
        _, (m2, peer) = axes(c)
        return rcopy(qall.at[c, m2], qall.at[c, m2], a2s.at[c, d - 1], a2r.at[c, d - 1], peer(d))

    def ag3(c, d):
        _, (m2, _) = axes(c)
        a = (m2 + side - d) % side
        return rcopy(qall.at[c, a], qall.at[c, side + a], a3s.at[c, d], a3r.at[c, d], sib)

    def od(c):
        return rcopy(osend.at[c % 2], orecv.at[c], ods.at[c], odr.at[c], sib)

    def rs1(c, d):
        _, (m2, peer) = axes(c)
        a = (m2 + d) % side
        return (rcopy(p1s.at[c, a], p1r.at[c, m2], s1.at[c, d - 1], r1.at[c, d - 1], peer(d)),
                rcopy(l1s.at[c], l1r.at[c, m2], sl1.at[c, d - 1], rl1.at[c, d - 1], peer(d)))

    def rs2(c, d):
        (m1, peer), _ = axes(c)
        a = (m1 + d) % side
        return (rcopy(p2s.at[c, a], p2r.at[c, m1], s2.at[c, d - 1], r2.at[c, d - 1], peer(d)),
                rcopy(l2s.at[c], l2r.at[c, m1], sl2.at[c, d - 1], rl2.at[c, d - 1], peer(d)))

    def cload(b):
        return pltpu.make_async_copy(cache_ref.at[b], cbuf.at[b % NBUF], csem.at[b % NBUF])

    for b in range(min(NBUF, total)):
        cload(b).start()

    barrier = pltpu.get_barrier_semaphore()
    peers = [sib] + [at(y, (x + d) % side, core) for d in dists] + [at((y + d) % side, x, core) for d in dists]
    for dev in peers:
        pl.semaphore_signal(barrier, inc=1, device_id=dev, device_id_type=pl.DeviceIdType.MESH)
    pl.semaphore_wait(barrier, len(peers))

    order = sorted(dists, key=lambda d: min(d, side - d))
    for c in range(nc):
        for d in order:
            ag1(c, d).start()

    def gather_first(c):
        (m1, _), (m2, _) = axes(c)
        g1[c, m1] = q_ref[pl.ds(c * nb, nb)]
        for d in order:
            ag1(c, d).wait_recv()

        def body(i, _):
            parts = [g1[c, a, i].astype(jnp.float32) for a in range(side)]
            qall[c, m2, i] = jnp.concatenate(parts, axis=0).astype(qall.dtype)
            return 0

        lax.fori_loop(0, nb, body, 0)
        for d in order:
            ag2(c, d).start()
        ag3(c, 0).start()

    def gather_second(c):
        for d in order:
            ag2(c, d).wait_recv()
            ag3(c, d).start()

    def gather_third(c):
        for d in range(side):
            ag3(c, d).wait_recv()

    tpos = lax.broadcasted_iota(jnp.int32, (1, t), 1)
    pos = (tpos // page) * (page * n) + me * page + tpos % page

    def compute(c):
        if c >= 2:
            od(c - 2).wait_send()

        def one(i, _):
            b = c * nb + i
            slot = b % NBUF
            cload(b).wait()
            qb = qall[c, :, i].reshape(2 * half, k)
            cb = cbuf[slot]
            s = lax.dot_general(qb, cb, (((1,), (1,)), ((), ())), preferred_element_type=jnp.float32)
            s = jnp.where(pos < lens_ref[b], s, NEG)
            m = jnp.max(s, axis=1, keepdims=True)
            ms = jnp.where(m == NEG, 0.0, m)
            p = jnp.exp((s - ms) * SCALE)
            l = jnp.sum(p, axis=1, keepdims=True)
            acc = lax.dot_general(p.astype(jnp.bfloat16), cb[:, :lorav], (((1,), (0,)), ((), ())),
                                  preferred_element_type=jnp.float32)
            ls = jnp.where(l > 0.0, l, 1.0)
            o = acc * (1.0 / ls)
            lse = jnp.broadcast_to(jnp.where(l > 0.0, ms * SCALE + jnp.log(ls), NEG), (2 * half, LANES))
            own[c % 2, i, :, :lorav] = o[:half]
            own[c % 2, i, :, lorav:] = lse[:half]
            osend[c % 2, i, :, :lorav] = o[half:]
            osend[c % 2, i, :, lorav:] = lse[half:]

            @pl.when(b + NBUF < total)
            def _():
                cload(b + NBUF).start()

            return 0

        lax.fori_loop(0, nb, one, 0)
        od(c).start()

    diag = lax.broadcasted_iota(jnp.int32, (half, LANES), 0) == lax.broadcasted_iota(jnp.int32, (half, LANES), 1)

    def pair(c):
        od(c).wait_recv()

        def one(i, _):
            la = own[c % 2, i, :, lorav:]
            lb = orecv[c, i, :, lorav:]
            top = jnp.maximum(la, lb)
            ts = jnp.where(top == NEG, 0.0, top)
            wa = jnp.exp(la - ts)
            wb = jnp.exp(lb - ts)
            ws = wa + wb
            wss = jnp.where(ws > 0.0, ws, 1.0)
            inv = 1.0 / wss
            wa = wa * inv
            wb = wb * inv
            for j in range(lorav // LANES):
                cols = slice(j * LANES, (j + 1) * LANES)
                v = (wa * own[c % 2, i, :, cols] + wb * orecv[c, i, :, cols]).astype(jnp.bfloat16)
                p1s[c, :, i, :, cols] = v.reshape(side, tile, LANES)
            lse = jnp.where(ws > 0.0, ts + jnp.log(wss), NEG)
            l1s[c, pl.ds(i, 1)] = jnp.sum(jnp.where(diag, lse, 0.0), axis=0, keepdims=True)
            return 0

        lax.fori_loop(0, nb, one, 0)
        for d in order:
            for cp in rs1(c, d):
                cp.start()

    def weights(ls):
        top = functools.reduce(jnp.maximum, ls)
        ts = jnp.where(top == NEG, 0.0, top)
        w = [jnp.exp(v - ts) for v in ls]
        ws = functools.reduce(jnp.add, w)
        wss = jnp.where(ws > 0.0, ws, 1.0)
        inv = 1.0 / wss
        for j, v in enumerate(w):
            wrow[j] = v * inv
        return jnp.where(ws > 0.0, ts + jnp.log(wss), NEG)

    def combine(i, rows, first, srcs):
        sel = (lax.broadcasted_iota(jnp.int32, (rows, LANES), 0) + first
               == lax.broadcasted_iota(jnp.int32, (rows, LANES), 1))
        tot = None
        for j, src in enumerate(srcs):
            w = jnp.broadcast_to(wrow[j, pl.ds(i, 1)], (rows, LANES))
            w = jnp.sum(jnp.where(sel, w, 0.0), axis=1, keepdims=True)
            term = w * src[i].astype(jnp.float32)
            tot = term if tot is None else tot + term
        return tot

    def second(c):
        (m1, _), (m2, _) = axes(c)
        for d in order:
            for cp in rs1(c, d):
                cp.wait_recv()
        idx = [(m2 + d) % side for d in dists]
        l2s[c] = weights([l1s[c]] + [l1r[c, a] for a in idx])
        srcs = [p1s.at[c, m2]] + [p1r.at[c, a] for a in idx]

        def one(i, _):
            v = combine(i, tile, m2 * tile, srcs)
            for a in range(side):
                p2s[c, a, i] = v[a * hl:(a + 1) * hl]
            return 0

        lax.fori_loop(0, nb, one, 0)
        for d in order:
            for cp in rs2(c, d):
                cp.start()

    def final(c):
        (m1, _), (m2, _) = axes(c)
        for d in order:
            for cp in rs2(c, d):
                cp.wait_recv()
        idx = [(m1 + d) % side for d in dists]
        weights([l2s[c]] + [l2r[c, a] for a in idx])
        srcs = [p2s.at[c, m1]] + [p2r.at[c, a] for a in idx]

        def one(i, _):
            out_ref[c * nb + i] = combine(i, hl, m2 * tile + m1 * hl, srcs).astype(out_ref.dtype)
            return 0

        lax.fori_loop(0, nb, one, 0)

    for c in range(nc):
        gather_first(c)
    gather_second(0)
    for c in range(nc + 3):
        if c + 1 < nc:
            gather_second(c + 1)
        if c < nc:
            gather_third(c)
            compute(c)
        if 0 <= c - 1 < nc:
            pair(c - 1)
        if 0 <= c - 2 < nc:
            second(c - 2)
        if 0 <= c - 3 < nc:
            final(c - 3)
    for c in range(nc):
        for d in dists:
            ag1(c, d).wait_send()
            ag2(c, d).wait_send()
            for cp in rs1(c, d) + rs2(c, d):
                cp.wait_send()
        for d in range(side):
            ag3(c, d).wait_send()
        if c >= nc - 2:
            od(c).wait_send()


def solution(mesh):
    n = mesh.shape['dcp']
    side = math.isqrt(n // 2)

    def local(q, cache, lens):
        b, hl, k = q.shape
        t = cache.shape[1] * cache.shape[3]
        lorav = k - ROPE
        nb = min(8, max(1, b // 2))
        nc = b // nb
        tile = side * hl
        half = side * tile
        bf, f32 = jnp.bfloat16, jnp.float32
        dma = pltpu.SemaphoreType.DMA
        return pl.pallas_call(
            functools.partial(kernel, n, side, nc, nb, cache.shape[3]),
            out_shape=jax.ShapeDtypeStruct((b, hl, lorav), bf),
            in_specs=[pl.BlockSpec(memory_space=pltpu.VMEM), pl.BlockSpec(memory_space=pl.ANY),
                      pl.BlockSpec(memory_space=pltpu.SMEM)],
            out_specs=pl.BlockSpec(memory_space=pltpu.VMEM),
            scratch_shapes=[
                pltpu.VMEM((nc, side, nb, hl, k), bf),
                pltpu.VMEM((nc, 2 * side, nb, tile, k), bf),
                pltpu.VMEM((NBUF, t, k), bf),
                pltpu.VMEM((2, nb, half, lorav + LANES), f32),
                pltpu.VMEM((2, nb, half, lorav + LANES), f32),
                pltpu.VMEM((nc, nb, half, lorav + LANES), f32),
                pltpu.VMEM((nc, side, nb, tile, lorav), bf),
                pltpu.VMEM((nc, side, nb, tile, lorav), bf),
                pltpu.VMEM((nc, nb, LANES), f32),
                pltpu.VMEM((nc, side, nb, LANES), f32),
                pltpu.VMEM((nc, side, nb, hl, lorav), f32),
                pltpu.VMEM((nc, side, nb, hl, lorav), f32),
                pltpu.VMEM((nc, nb, LANES), f32),
                pltpu.VMEM((nc, side, nb, LANES), f32),
                pltpu.VMEM((side, nb, LANES), f32),
                dma((NBUF,)),
                dma((nc, side - 1)), dma((nc, side - 1)),
                dma((nc, side - 1)), dma((nc, side - 1)),
                dma((nc, side)), dma((nc, side)),
                dma((nc,)), dma((nc,)),
                dma((nc, side - 1)), dma((nc, side - 1)), dma((nc, side - 1)), dma((nc, side - 1)),
                dma((nc, side - 1)), dma((nc, side - 1)), dma((nc, side - 1)), dma((nc, side - 1)),
            ],
            compiler_params=pltpu.CompilerParams(collective_id=0, has_side_effects=True,
                                                 vmem_limit_bytes=63 * 1024 * 1024),
        )(q, cache.reshape(b, t, k), lens)

    return jax.shard_map(local, mesh=mesh, in_specs=(P('dp', 'dcp', None), P('dp', None, 'dcp', None, None), P('dp')),
                         out_specs=P('dp', 'dcp', None), check_vma=False)
```

```python
import functools
import math

import jax
import jax.numpy as jnp
from jax import lax
from jax.experimental import pallas as pl
from jax.experimental.pallas import tpu as pltpu
from jax.sharding import PartitionSpec as P

ROPE = 64
QK_DIM = 192
SCALE = QK_DIM ** -0.5
NEG = float('-inf')
LANES = 128
NBUF = 4


def kernel(n, side, nc, nb, page, q_ref, cache_ref, lens_ref, out_ref,
           g1, qall, cbuf, own, osend, orecv, p1s, p1x, p1r, l1s, l1r, p2s, p2x, p2r, l2s, l2r, wrow,
           csem, a1s, a1r, a2s, a2r, a3s, a3r, ods, odr, s1, r1, sl1, rr1, s2, r2, sl2, rr2):
    hl = q_ref.shape[1]
    k = q_ref.shape[2]
    t = cbuf.shape[1]
    lorav = k - ROPE
    tile = side * hl
    half = side * tile
    total = nc * nb

    me = lax.axis_index('dcp')
    core = me % 2
    x = (me // 2) % side
    y = me // (2 * side)
    dists = tuple(range(1, side))

    def at(yy, xx, cc):
        return {'dcp': (yy * side + xx) * 2 + cc}

    sib = at(y, x, 1 - core)

    def axes(c):
        ax = (x, lambda d: at(y, (x + d) % side, core))
        ay = (y, lambda d: at((y + d) % side, x, core))
        return (ax, ay) if c % 2 == 0 else (ay, ax)

    def rcopy(src, dst, ss, rs, dev):
        return pltpu.make_async_remote_copy(src_ref=src, dst_ref=dst, send_sem=ss, recv_sem=rs, device_id=dev,
                                            device_id_type=pl.DeviceIdType.MESH)

    hb = nb // 2

    def part(h):
        return pl.ds(h * hb, hb)

    near = (1, side - 1)

    def ag1(c, h):
        (m1, peer), _ = axes(c)
        return rcopy(q_ref.at[pl.ds(c * nb, nb)], g1.at[c, m1], a1s.at[c, h], a1r.at[c, h], peer(near[h]))

    def ag1f(c, h):
        (m1, peer), _ = axes(c)
        a = (m1 + side - near[h]) % side
        return rcopy(g1.at[c, a, part(h)], g1.at[c, a, part(h)], a1s.at[c, 2 + h], a1r.at[c, 2 + h], peer(near[h]))

    def ag2(c, h):
        _, (m2, peer) = axes(c)
        return rcopy(qall.at[c, m2], qall.at[c, m2], a2s.at[c, h], a2r.at[c, h], peer(near[h]))

    def ag2f(c, h):
        _, (m2, peer) = axes(c)
        a = (m2 + side - near[h]) % side
        return rcopy(qall.at[c, a, part(h)], qall.at[c, a, part(h)], a2s.at[c, 2 + h], a2r.at[c, 2 + h], peer(near[h]))

    def ag3(c, d):
        _, (m2, _) = axes(c)
        a = (m2 + side - d) % side
        return rcopy(qall.at[c, a], qall.at[c, side + a], a3s.at[c, d], a3r.at[c, d], sib)

    def od(c):
        return rcopy(osend.at[c % 2], orecv.at[c], ods.at[c], odr.at[c], sib)

    def rs1(c, h):
        _, (m2, peer) = axes(c)
        return rcopy(p1s.at[c, (m2 + near[h]) % side], p1r.at[c, m2], s1.at[c, h], r1.at[c, h], peer(near[h]))

    def rs1x(c, h):
        _, (m2, peer) = axes(c)
        return rcopy(p1s.at[c, (m2 + 2) % side, part(h)], p1x.at[c, h], s1.at[c, 2 + h], r1.at[c, 2 + h], peer(near[h]))

    def rs1f(c, h):
        _, (m2, peer) = axes(c)
        a = (m2 + side - near[h]) % side
        return rcopy(p1x.at[c, h], p1r.at[c, a, part(h)], s1.at[c, 4 + h], r1.at[c, 4 + h], peer(near[h]))

    def rl1(c, d):
        _, (m2, peer) = axes(c)
        return rcopy(l1s.at[c], l1r.at[c, m2], sl1.at[c, d - 1], rr1.at[c, d - 1], peer(d))

    def rs2(c, h):
        (m1, peer), _ = axes(c)
        return rcopy(p2s.at[c, (m1 + near[h]) % side], p2r.at[c, m1], s2.at[c, h], r2.at[c, h], peer(near[h]))

    def rs2x(c, h):
        (m1, peer), _ = axes(c)
        return rcopy(p2s.at[c, (m1 + 2) % side, part(h)], p2x.at[c, h], s2.at[c, 2 + h], r2.at[c, 2 + h], peer(near[h]))

    def rs2f(c, h):
        (m1, peer), _ = axes(c)
        a = (m1 + side - near[h]) % side
        return rcopy(p2x.at[c, h], p2r.at[c, a, part(h)], s2.at[c, 4 + h], r2.at[c, 4 + h], peer(near[h]))

    def rl2(c, d):
        (m1, peer), _ = axes(c)
        return rcopy(l2s.at[c], l2r.at[c, m1], sl2.at[c, d - 1], rr2.at[c, d - 1], peer(d))

    def cload(b):
        return pltpu.make_async_copy(cache_ref.at[b], cbuf.at[b % NBUF], csem.at[b % NBUF])

    for b in range(min(NBUF, total)):
        cload(b).start()

    barrier = pltpu.get_barrier_semaphore()
    peers = [sib] + [at(y, (x + d) % side, core) for d in dists] + [at((y + d) % side, x, core) for d in dists]
    for dev in peers:
        pl.semaphore_signal(barrier, inc=1, device_id=dev, device_id_type=pl.DeviceIdType.MESH)
    pl.semaphore_wait(barrier, len(peers))

    for c in range(nc):
        for h in range(2):
            ag1(c, h).start()
    for c in range(nc):
        for h in range(2):
            ag1(c, h).wait_recv()
            ag1f(c, h).start()

    def gather_first(c):
        (m1, _), (m2, _) = axes(c)
        g1[c, m1] = q_ref[pl.ds(c * nb, nb)]
        for h in range(2):
            ag1f(c, h).wait_recv()

        def body(i, _):
            parts = [g1[c, a, i].astype(jnp.float32) for a in range(side)]
            qall[c, m2, i] = jnp.concatenate(parts, axis=0).astype(qall.dtype)
            return 0

        lax.fori_loop(0, nb, body, 0)
        for h in range(2):
            ag2(c, h).start()
        ag3(c, 0).start()

    def gather_second(c):
        for h in range(2):
            ag2(c, h).wait_recv()
            ag2f(c, h).start()
            ag3(c, near[h]).start()

    def gather_far(c):
        for h in range(2):
            ag2f(c, h).wait_recv()
        ag3(c, 2).start()

    def gather_third(c):
        for d in range(side):
            ag3(c, d).wait_recv()

    tpos = lax.broadcasted_iota(jnp.int32, (1, t), 1)
    pos = (tpos // page) * (page * n) + me * page + tpos % page

    def compute(c):
        if c >= 2:
            od(c - 2).wait_send()

        def one(i, _):
            b = c * nb + i
            slot = b % NBUF
            cload(b).wait()
            qb = qall[c, :, i].reshape(2 * half, k)
            cb = cbuf[slot]
            s = lax.dot_general(qb, cb, (((1,), (1,)), ((), ())), preferred_element_type=jnp.float32)
            s = jnp.where(pos < lens_ref[b], s, NEG)
            m = jnp.max(s, axis=1, keepdims=True)
            ms = jnp.where(m == NEG, 0.0, m)
            p = jnp.exp((s - ms) * SCALE)
            l = jnp.sum(p, axis=1, keepdims=True)
            acc = lax.dot_general(p.astype(jnp.bfloat16), cb[:, :lorav], (((1,), (0,)), ((), ())),
                                  preferred_element_type=jnp.float32)
            ls = jnp.where(l > 0.0, l, 1.0)
            o = acc * (1.0 / ls)
            lse = jnp.broadcast_to(jnp.where(l > 0.0, ms * SCALE + jnp.log(ls), NEG), (2 * half, LANES))
            own[c % 2, i, :, :lorav] = o[:half]
            own[c % 2, i, :, lorav:] = lse[:half]
            osend[c % 2, i, :, :lorav] = o[half:]
            osend[c % 2, i, :, lorav:] = lse[half:]

            @pl.when(b + NBUF < total)
            def _():
                cload(b + NBUF).start()

            return 0

        lax.fori_loop(0, nb, one, 0)
        od(c).start()

    diag = lax.broadcasted_iota(jnp.int32, (half, LANES), 0) == lax.broadcasted_iota(jnp.int32, (half, LANES), 1)

    def pair(c):
        od(c).wait_recv()

        def one(i, _):
            la = own[c % 2, i, :, lorav:]
            lb = orecv[c, i, :, lorav:]
            top = jnp.maximum(la, lb)
            ts = jnp.where(top == NEG, 0.0, top)
            wa = jnp.exp(la - ts)
            wb = jnp.exp(lb - ts)
            ws = wa + wb
            wss = jnp.where(ws > 0.0, ws, 1.0)
            inv = 1.0 / wss
            wa = wa * inv
            wb = wb * inv
            for j in range(lorav // LANES):
                cols = slice(j * LANES, (j + 1) * LANES)
                v = (wa * own[c % 2, i, :, cols] + wb * orecv[c, i, :, cols]).astype(jnp.bfloat16)
                p1s[c, :, i, :, cols] = v.reshape(side, tile, LANES)
            lse = jnp.where(ws > 0.0, ts + jnp.log(wss), NEG)
            l1s[c, pl.ds(i, 1)] = jnp.sum(jnp.where(diag, lse, 0.0), axis=0, keepdims=True)
            return 0

        lax.fori_loop(0, nb, one, 0)
        for h in range(2):
            rs1x(c, h).start()
        for d in dists:
            rl1(c, d).start()
        for h in range(2):
            rs1(c, h).start()

    def pair_relay(c):
        for h in range(2):
            rs1x(c, h).wait_recv()
            rs1f(c, h).start()

    def weights(ls):
        top = functools.reduce(jnp.maximum, ls)
        ts = jnp.where(top == NEG, 0.0, top)
        w = [jnp.exp(v - ts) for v in ls]
        ws = functools.reduce(jnp.add, w)
        wss = jnp.where(ws > 0.0, ws, 1.0)
        inv = 1.0 / wss
        for j, v in enumerate(w):
            wrow[j] = v * inv
        return jnp.where(ws > 0.0, ts + jnp.log(wss), NEG)

    def combine(i, rows, first, srcs):
        sel = (lax.broadcasted_iota(jnp.int32, (rows, LANES), 0) + first
               == lax.broadcasted_iota(jnp.int32, (rows, LANES), 1))
        tot = None
        for j, src in enumerate(srcs):
            w = jnp.broadcast_to(wrow[j, pl.ds(i, 1)], (rows, LANES))
            w = jnp.sum(jnp.where(sel, w, 0.0), axis=1, keepdims=True)
            term = w * src[i].astype(jnp.float32)
            tot = term if tot is None else tot + term
        return tot

    def second(c):
        (m1, _), (m2, _) = axes(c)
        for h in range(2):
            rs1(c, h).wait_recv()
            rs1f(c, h).wait_recv()
        for d in dists:
            rl1(c, d).wait_recv()
        idx = [(m2 + d) % side for d in dists]
        l2s[c] = weights([l1s[c]] + [l1r[c, a] for a in idx])
        srcs = [p1s.at[c, m2]] + [p1r.at[c, a] for a in idx]

        def one(i, _):
            v = combine(i, tile, m2 * tile, srcs)
            for a in range(side):
                p2s[c, a, i] = v[a * hl:(a + 1) * hl]
            return 0

        lax.fori_loop(0, nb, one, 0)
        for h in range(2):
            rs2x(c, h).start()
        for d in dists:
            rl2(c, d).start()
        for h in range(2):
            rs2(c, h).start()

    def second_relay(c):
        for h in range(2):
            rs2x(c, h).wait_recv()
            rs2f(c, h).start()

    def final(c):
        (m1, _), (m2, _) = axes(c)
        for h in range(2):
            rs2(c, h).wait_recv()
            rs2f(c, h).wait_recv()
        for d in dists:
            rl2(c, d).wait_recv()
        idx = [(m1 + d) % side for d in dists]
        weights([l2s[c]] + [l2r[c, a] for a in idx])
        srcs = [p2s.at[c, m1]] + [p2r.at[c, a] for a in idx]

        def one(i, _):
            out_ref[c * nb + i] = combine(i, hl, m2 * tile + m1 * hl, srcs).astype(out_ref.dtype)
            return 0

        lax.fori_loop(0, nb, one, 0)

    stages = ((gather_first, 6), (gather_second, 4), (gather_far, 1), (gather_third, 0), (compute, 0), (pair, -1),
              (pair_relay, -2), (second, -3), (second_relay, -4), (final, -5))
    for c in range(-6, nc + 5):
        for stage, ahead in stages:
            if 0 <= c + ahead < nc:
                stage(c + ahead)

    for c in range(nc):
        for h in range(2):
            for cp in (ag1, ag1f, ag2, ag2f, rs1, rs1x, rs1f, rs2, rs2x, rs2f):
                cp(c, h).wait_send()
        for d in dists:
            rl1(c, d).wait_send()
            rl2(c, d).wait_send()
        for d in range(side):
            ag3(c, d).wait_send()
        if c >= nc - 2:
            od(c).wait_send()


def solution(mesh):
    n = mesh.shape['dcp']
    side = math.isqrt(n // 2)

    def local(q, cache, lens):
        b, hl, k = q.shape
        t = cache.shape[1] * cache.shape[3]
        lorav = k - ROPE
        nb = min(8, max(1, b // 2))
        nc = b // nb
        tile = side * hl
        half = side * tile
        bf, f32 = jnp.bfloat16, jnp.float32
        dma = pltpu.SemaphoreType.DMA
        return pl.pallas_call(
            functools.partial(kernel, n, side, nc, nb, cache.shape[3]),
            out_shape=jax.ShapeDtypeStruct((b, hl, lorav), bf),
            in_specs=[pl.BlockSpec(memory_space=pltpu.VMEM), pl.BlockSpec(memory_space=pl.ANY),
                      pl.BlockSpec(memory_space=pltpu.SMEM)],
            out_specs=pl.BlockSpec(memory_space=pltpu.VMEM),
            scratch_shapes=[
                pltpu.VMEM((nc, side, nb, hl, k), bf),
                pltpu.VMEM((nc, 2 * side, nb, tile, k), bf),
                pltpu.VMEM((NBUF, t, k), bf),
                pltpu.VMEM((2, nb, half, lorav + LANES), f32),
                pltpu.VMEM((2, nb, half, lorav + LANES), f32),
                pltpu.VMEM((nc, nb, half, lorav + LANES), f32),
                pltpu.VMEM((nc, side, nb, tile, lorav), bf),
                pltpu.VMEM((nc, 2, nb // 2, tile, lorav), bf),
                pltpu.VMEM((nc, side, nb, tile, lorav), bf),
                pltpu.VMEM((nc, nb, LANES), f32),
                pltpu.VMEM((nc, side, nb, LANES), f32),
                pltpu.VMEM((nc, side, nb, hl, lorav), f32),
                pltpu.VMEM((nc, 2, nb // 2, hl, lorav), f32),
                pltpu.VMEM((nc, side, nb, hl, lorav), f32),
                pltpu.VMEM((nc, nb, LANES), f32),
                pltpu.VMEM((nc, side, nb, LANES), f32),
                pltpu.VMEM((side, nb, LANES), f32),
                dma((NBUF,)),
                dma((nc, 4)), dma((nc, 4)), dma((nc, 4)), dma((nc, 4)),
                dma((nc, side)), dma((nc, side)),
                dma((nc,)), dma((nc,)),
                dma((nc, 6)), dma((nc, 6)), dma((nc, side - 1)), dma((nc, side - 1)),
                dma((nc, 6)), dma((nc, 6)), dma((nc, side - 1)), dma((nc, side - 1)),
            ],
            compiler_params=pltpu.CompilerParams(collective_id=0, has_side_effects=True,
                                                 vmem_limit_bytes=63 * 1024 * 1024),
        )(q, cache.reshape(b, t, k), lens)

    return jax.shard_map(local, mesh=mesh, in_specs=(P('dp', 'dcp', None), P('dp', None, 'dcp', None, None), P('dp')),
                         out_specs=P('dp', 'dcp', None), check_vma=False)
```

```python
import functools
import math

import jax
import jax.numpy as jnp
from jax import lax
from jax.experimental import pallas as pl
from jax.experimental.pallas import tpu as pltpu
from jax.sharding import PartitionSpec as P

ROPE = 64
QK_DIM = 192
SCALE = QK_DIM ** -0.5
NEG = float('-inf')
LANES = 128
NBUF = 4
NSLOT = 4


def kernel(n, side, nc, nb, page, q_ref, cache_ref, lens_ref, out_ref,
           g1, qall, cbuf, own, osend, orecv, p1s, p1x, p1r, l1s, l1r, p2s, p2x, p2r, l2s, l2r, wrow,
           csem, a1s, a1r, a2s, a2r, a3s, a3r, ods, odr, s1, r1, sl1, rr1, s2, r2, sl2, rr2):
    hl = q_ref.shape[1]
    k = q_ref.shape[2]
    t = cbuf.shape[1]
    lorav = k - ROPE
    tile = side * hl
    half = side * tile
    total = nc * nb

    me = lax.axis_index('dcp')
    core = me % 2
    x = (me // 2) % side
    y = me // (2 * side)
    dists = tuple(range(1, side))

    def at(yy, xx, cc):
        return {'dcp': (yy * side + xx) * 2 + cc}

    sib = at(y, x, 1 - core)

    def axes(c):
        odd = c % 2
        return ((x + odd * (y - x), lambda d: at((y + odd * d) % side, (x + (1 - odd) * d) % side, core)),
                (y + odd * (x - y), lambda d: at((y + (1 - odd) * d) % side, (x + odd * d) % side, core)))

    def rcopy(src, dst, ss, rs, dev):
        return pltpu.make_async_remote_copy(src_ref=src, dst_ref=dst, send_sem=ss, recv_sem=rs, device_id=dev,
                                            device_id_type=pl.DeviceIdType.MESH)

    hb = nb // 2

    def part(h):
        return pl.ds(h * hb, hb)

    near = (1, side - 1)

    def ag1(c, h):
        (m1, peer), _ = axes(c)
        return rcopy(q_ref.at[pl.ds(c * nb, nb)], g1.at[c, m1], a1s.at[c, h], a1r.at[c, h], peer(near[h]))

    def ag1f(c, h):
        (m1, peer), _ = axes(c)
        a = (m1 + side - near[h]) % side
        return rcopy(g1.at[c, a, part(h)], g1.at[c, a, part(h)], a1s.at[c, 2 + h], a1r.at[c, 2 + h], peer(near[h]))

    def ag2(c, h):
        _, (m2, peer) = axes(c)
        return rcopy(qall.at[c, m2], qall.at[c, m2], a2s.at[c, h], a2r.at[c, h], peer(near[h]))

    def ag2f(c, h):
        _, (m2, peer) = axes(c)
        a = (m2 + side - near[h]) % side
        return rcopy(qall.at[c, a, part(h)], qall.at[c, a, part(h)], a2s.at[c, 2 + h], a2r.at[c, 2 + h], peer(near[h]))

    def ag3(c, d):
        _, (m2, _) = axes(c)
        a = (m2 + side - d) % side
        return rcopy(qall.at[c, a], qall.at[c, side + a], a3s.at[c, d], a3r.at[c, d], sib)

    def od(c):
        return rcopy(osend.at[c % NSLOT], orecv.at[c], ods.at[c], odr.at[c], sib)

    def rs1(c, h):
        _, (m2, peer) = axes(c)
        return rcopy(p1s.at[c, (m2 + near[h]) % side], p1r.at[c, m2], s1.at[c, h], r1.at[c, h], peer(near[h]))

    def rs1x(c, h):
        _, (m2, peer) = axes(c)
        return rcopy(p1s.at[c, (m2 + 2) % side, part(h)], p1x.at[c, h], s1.at[c, 2 + h], r1.at[c, 2 + h], peer(near[h]))

    def rs1f(c, h):
        _, (m2, peer) = axes(c)
        a = (m2 + side - near[h]) % side
        return rcopy(p1x.at[c, h], p1r.at[c, a, part(h)], s1.at[c, 4 + h], r1.at[c, 4 + h], peer(near[h]))

    def rl1(c, d):
        _, (m2, peer) = axes(c)
        return rcopy(l1s.at[c], l1r.at[c, m2], sl1.at[c, d - 1], rr1.at[c, d - 1], peer(d))

    def rs2(c, h):
        (m1, peer), _ = axes(c)
        return rcopy(p2s.at[c, (m1 + near[h]) % side], p2r.at[c, m1], s2.at[c, h], r2.at[c, h], peer(near[h]))

    def rs2x(c, h):
        (m1, peer), _ = axes(c)
        return rcopy(p2s.at[c, (m1 + 2) % side, part(h)], p2x.at[c, h], s2.at[c, 2 + h], r2.at[c, 2 + h], peer(near[h]))

    def rs2f(c, h):
        (m1, peer), _ = axes(c)
        a = (m1 + side - near[h]) % side
        return rcopy(p2x.at[c, h], p2r.at[c, a, part(h)], s2.at[c, 4 + h], r2.at[c, 4 + h], peer(near[h]))

    def rl2(c, d):
        (m1, peer), _ = axes(c)
        return rcopy(l2s.at[c], l2r.at[c, m1], sl2.at[c, d - 1], rr2.at[c, d - 1], peer(d))

    def cload(b):
        return pltpu.make_async_copy(cache_ref.at[b], cbuf.at[b % NBUF], csem.at[b % NBUF])

    for b in range(min(NBUF, total)):
        cload(b).start()

    barrier = pltpu.get_barrier_semaphore()
    peers = [sib] + [at(y, (x + d) % side, core) for d in dists] + [at((y + d) % side, x, core) for d in dists]
    for dev in peers:
        pl.semaphore_signal(barrier, inc=1, device_id=dev, device_id_type=pl.DeviceIdType.MESH)
    pl.semaphore_wait(barrier, len(peers))

    def gather_start(c):
        for h in range(2):
            ag1(c, h).start()

    def gather_relay(c):
        for h in range(2):
            ag1(c, h).wait_recv()
            ag1f(c, h).start()

    def gather_first(c):
        (m1, _), (m2, _) = axes(c)
        g1[c, m1] = q_ref[pl.ds(c * nb, nb)]
        for h in range(2):
            ag1f(c, h).wait_recv()

        def body(i, _):
            parts = [g1[c, a, i].astype(jnp.float32) for a in range(side)]
            qall[c, m2, i] = jnp.concatenate(parts, axis=0).astype(qall.dtype)
            return 0

        lax.fori_loop(0, nb, body, 0)
        for h in range(2):
            ag2(c, h).start()
        ag3(c, 0).start()

    def gather_second(c):
        for h in range(2):
            ag2(c, h).wait_recv()
            ag2f(c, h).start()
            ag3(c, near[h]).start()

    def gather_far(c):
        for h in range(2):
            ag2f(c, h).wait_recv()
        ag3(c, 2).start()

    def gather_third(c):
        for d in range(side):
            ag3(c, d).wait_recv()

    tpos = lax.broadcasted_iota(jnp.int32, (1, t), 1)
    pos = (tpos // page) * (page * n) + me * page + tpos % page

    def compute(c):
        @pl.when(c >= NSLOT)
        def _():
            od(c - NSLOT).wait_send()

        def one(i, _):
            b = c * nb + i
            slot = b % NBUF
            cload(b).wait()
            qb = qall[c, :, i].reshape(2 * half, k)
            cb = cbuf[slot]
            s = lax.dot_general(qb, cb, (((1,), (1,)), ((), ())), preferred_element_type=jnp.float32)
            s = jnp.where(pos < lens_ref[b], s, NEG)
            m = jnp.max(s, axis=1, keepdims=True)
            ms = jnp.where(m == NEG, 0.0, m)
            p = jnp.exp((s - ms) * SCALE)
            l = jnp.sum(p, axis=1, keepdims=True)
            acc = lax.dot_general(p.astype(jnp.bfloat16), cb[:, :lorav], (((1,), (0,)), ((), ())),
                                  preferred_element_type=jnp.float32)
            ls = jnp.where(l > 0.0, l, 1.0)
            o = acc * (1.0 / ls)
            lse = jnp.broadcast_to(jnp.where(l > 0.0, ms * SCALE + jnp.log(ls), NEG), (2 * half, LANES))
            own[c % NSLOT, i, :, :lorav] = o[:half]
            own[c % NSLOT, i, :, lorav:] = lse[:half]
            osend[c % NSLOT, i, :, :lorav] = o[half:]
            osend[c % NSLOT, i, :, lorav:] = lse[half:]

            @pl.when(b + NBUF < total)
            def _():
                cload(b + NBUF).start()

            return 0

        lax.fori_loop(0, nb, one, 0)
        od(c).start()

    diag = lax.broadcasted_iota(jnp.int32, (half, LANES), 0) == lax.broadcasted_iota(jnp.int32, (half, LANES), 1)

    def pair(c):
        od(c).wait_recv()

        def one(i, _):
            la = own[c % NSLOT, i, :, lorav:]
            lb = orecv[c, i, :, lorav:]
            top = jnp.maximum(la, lb)
            ts = jnp.where(top == NEG, 0.0, top)
            wa = jnp.exp(la - ts)
            wb = jnp.exp(lb - ts)
            ws = wa + wb
            wss = jnp.where(ws > 0.0, ws, 1.0)
            inv = 1.0 / wss
            wa = wa * inv
            wb = wb * inv
            for j in range(lorav // LANES):
                cols = slice(j * LANES, (j + 1) * LANES)
                v = (wa * own[c % NSLOT, i, :, cols] + wb * orecv[c, i, :, cols]).astype(jnp.bfloat16)
                p1s[c, :, i, :, cols] = v.reshape(side, tile, LANES)
            lse = jnp.where(ws > 0.0, ts + jnp.log(wss), NEG)
            l1s[c, pl.ds(i, 1)] = jnp.sum(jnp.where(diag, lse, 0.0), axis=0, keepdims=True)
            return 0

        lax.fori_loop(0, nb, one, 0)
        for h in range(2):
            rs1x(c, h).start()
        for d in dists:
            rl1(c, d).start()
        for h in range(2):
            rs1(c, h).start()

    def pair_relay(c):
        for h in range(2):
            rs1x(c, h).wait_recv()
            rs1f(c, h).start()

    def weights(ls):
        top = functools.reduce(jnp.maximum, ls)
        ts = jnp.where(top == NEG, 0.0, top)
        w = [jnp.exp(v - ts) for v in ls]
        ws = functools.reduce(jnp.add, w)
        wss = jnp.where(ws > 0.0, ws, 1.0)
        inv = 1.0 / wss
        for j, v in enumerate(w):
            wrow[j] = v * inv
        return jnp.where(ws > 0.0, ts + jnp.log(wss), NEG)

    def combine(i, rows, first, srcs):
        sel = (lax.broadcasted_iota(jnp.int32, (rows, LANES), 0) + first
               == lax.broadcasted_iota(jnp.int32, (rows, LANES), 1))
        tot = None
        for j, src in enumerate(srcs):
            w = jnp.broadcast_to(wrow[j, pl.ds(i, 1)], (rows, LANES))
            w = jnp.sum(jnp.where(sel, w, 0.0), axis=1, keepdims=True)
            term = w * src[i].astype(jnp.float32)
            tot = term if tot is None else tot + term
        return tot

    def second(c):
        (m1, _), (m2, _) = axes(c)
        for h in range(2):
            rs1(c, h).wait_recv()
            rs1f(c, h).wait_recv()
        for d in dists:
            rl1(c, d).wait_recv()
        idx = [(m2 + d) % side for d in dists]
        l2s[c] = weights([l1s[c]] + [l1r[c, a] for a in idx])
        srcs = [p1s.at[c, m2]] + [p1r.at[c, a] for a in idx]

        def one(i, _):
            v = combine(i, tile, m2 * tile, srcs)
            for a in range(side):
                p2s[c, a, i] = v[a * hl:(a + 1) * hl]
            return 0

        lax.fori_loop(0, nb, one, 0)
        for h in range(2):
            rs2x(c, h).start()
        for d in dists:
            rl2(c, d).start()
        for h in range(2):
            rs2(c, h).start()

    def second_relay(c):
        for h in range(2):
            rs2x(c, h).wait_recv()
            rs2f(c, h).start()

    def final(c):
        (m1, _), (m2, _) = axes(c)
        for h in range(2):
            rs2(c, h).wait_recv()
            rs2f(c, h).wait_recv()
        for d in dists:
            rl2(c, d).wait_recv()
        idx = [(m1 + d) % side for d in dists]
        weights([l2s[c]] + [l2r[c, a] for a in idx])
        srcs = [p2s.at[c, m1]] + [p2r.at[c, a] for a in idx]

        def one(i, _):
            out_ref[c * nb + i] = combine(i, hl, m2 * tile + m1 * hl, srcs).astype(out_ref.dtype)
            return 0

        lax.fori_loop(0, nb, one, 0)

    def each(stage):
        def one(c, _):
            stage(c)
            return 0

        lax.fori_loop(0, nc, one, 0)

    each(gather_start)
    each(gather_relay)

    stages = ((gather_first, 0), (gather_second, 6), (gather_far, 12), (gather_third, 14), (compute, 14), (pair, 16),
              (pair_relay, 19), (second, 22), (second_relay, 26), (final, 30))

    def step(i, _):
        for stage, delay in stages:
            @pl.when((i >= delay) & (i < delay + nc))
            def _():
                stage(jnp.maximum(i - delay, 0))

        return 0

    lax.fori_loop(0, nc + stages[-1][1], step, 0)

    def drain(c):
        for h in range(2):
            for cp in (ag1, ag1f, ag2, ag2f, rs1, rs1x, rs1f, rs2, rs2x, rs2f):
                cp(c, h).wait_send()
        for d in dists:
            rl1(c, d).wait_send()
            rl2(c, d).wait_send()
        for d in range(side):
            ag3(c, d).wait_send()

        @pl.when(c >= nc - NSLOT)
        def _():
            od(c).wait_send()

    each(drain)


def solution(mesh):
    n = mesh.shape['dcp']
    side = math.isqrt(n // 2)

    def local(q, cache, lens):
        b, hl, k = q.shape
        t = cache.shape[1] * cache.shape[3]
        lorav = k - ROPE
        nb = min(4, max(1, b // 2))
        nc = b // nb
        tile = side * hl
        half = side * tile
        bf, f32 = jnp.bfloat16, jnp.float32
        dma = pltpu.SemaphoreType.DMA
        return pl.pallas_call(
            functools.partial(kernel, n, side, nc, nb, cache.shape[3]),
            out_shape=jax.ShapeDtypeStruct((b, hl, lorav), bf),
            in_specs=[pl.BlockSpec(memory_space=pltpu.VMEM), pl.BlockSpec(memory_space=pl.ANY),
                      pl.BlockSpec(memory_space=pltpu.SMEM)],
            out_specs=pl.BlockSpec(memory_space=pltpu.VMEM),
            scratch_shapes=[
                pltpu.VMEM((nc, side, nb, hl, k), bf),
                pltpu.VMEM((nc, 2 * side, nb, tile, k), bf),
                pltpu.VMEM((NBUF, t, k), bf),
                pltpu.VMEM((NSLOT, nb, half, lorav + LANES), f32),
                pltpu.VMEM((NSLOT, nb, half, lorav + LANES), f32),
                pltpu.VMEM((nc, nb, half, lorav + LANES), f32),
                pltpu.VMEM((nc, side, nb, tile, lorav), bf),
                pltpu.VMEM((nc, 2, nb // 2, tile, lorav), bf),
                pltpu.VMEM((nc, side, nb, tile, lorav), bf),
                pltpu.VMEM((nc, nb, LANES), f32),
                pltpu.VMEM((nc, side, nb, LANES), f32),
                pltpu.VMEM((nc, side, nb, hl, lorav), f32),
                pltpu.VMEM((nc, 2, nb // 2, hl, lorav), f32),
                pltpu.VMEM((nc, side, nb, hl, lorav), f32),
                pltpu.VMEM((nc, nb, LANES), f32),
                pltpu.VMEM((nc, side, nb, LANES), f32),
                pltpu.VMEM((side, nb, LANES), f32),
                dma((NBUF,)),
                dma((nc, 4)), dma((nc, 4)), dma((nc, 4)), dma((nc, 4)),
                dma((nc, side)), dma((nc, side)),
                dma((nc,)), dma((nc,)),
                dma((nc, 6)), dma((nc, 6)), dma((nc, side - 1)), dma((nc, side - 1)),
                dma((nc, 6)), dma((nc, 6)), dma((nc, side - 1)), dma((nc, side - 1)),
            ],
            compiler_params=pltpu.CompilerParams(collective_id=0, has_side_effects=True,
                                                 vmem_limit_bytes=63 * 1024 * 1024),
        )(q, cache.reshape(b, t, k), lens)

    return jax.shard_map(local, mesh=mesh, in_specs=(P('dp', 'dcp', None), P('dp', None, 'dcp', None, None), P('dp')),
                         out_specs=P('dp', 'dcp', None), check_vma=False)
```

```python
import functools
import math

import jax
import jax.numpy as jnp
from jax import lax
from jax.experimental import pallas as pl
from jax.experimental.pallas import tpu as pltpu
from jax.sharding import PartitionSpec as P

ROPE = 64
QK_DIM = 192
SCALE = QK_DIM ** -0.5
NEG = float('-inf')
LANES = 128
NBUF = 6
NSLOT = 4


def kernel(n, side, nc, nb, page, q_ref, cache_ref, lens_ref, out_ref,
           g1, qall, cbuf, own, osend, orecv, p1s, p1x, p1r, l1s, l1r, p2s, p2x, p2r, l2s, l2r, wrow, sb0, sb1,
           csem, a1s, a1r, a2s, a2r, a3s, a3r, ods, odr, s1, r1, sl1, rr1, s2, r2, sl2, rr2):
    hl = q_ref.shape[1]
    k = q_ref.shape[2]
    t = cbuf.shape[1]
    lorav = k - ROPE
    tile = side * hl
    half = side * tile
    total = nc * nb

    me = lax.axis_index('dcp')
    core = me % 2
    x = (me // 2) % side
    y = me // (2 * side)
    dists = tuple(range(1, side))

    def at(yy, xx, cc):
        return {'dcp': (yy * side + xx) * 2 + cc}

    sib = at(y, x, 1 - core)

    def axes(c):
        odd = c % 2
        return ((x + odd * (y - x), lambda d: at((y + odd * d) % side, (x + (1 - odd) * d) % side, core)),
                (y + odd * (x - y), lambda d: at((y + (1 - odd) * d) % side, (x + odd * d) % side, core)))

    def rcopy(src, dst, ss, rs, dev):
        return pltpu.make_async_remote_copy(src_ref=src, dst_ref=dst, send_sem=ss, recv_sem=rs, device_id=dev,
                                            device_id_type=pl.DeviceIdType.MESH)

    hb = nb // 2

    def part(h):
        return pl.ds(h * hb, hb)

    near = (1, side - 1)

    def ag1(c, h):
        (m1, peer), _ = axes(c)
        return rcopy(q_ref.at[pl.ds(c * nb, nb)], g1.at[c, m1], a1s.at[c, h], a1r.at[c, h], peer(near[h]))

    def ag1f(c, h):
        (m1, peer), _ = axes(c)
        a = (m1 + side - near[h]) % side
        return rcopy(g1.at[c, a, part(h)], g1.at[c, a, part(h)], a1s.at[c, 2 + h], a1r.at[c, 2 + h], peer(near[h]))

    def ag2(c, h):
        _, (m2, peer) = axes(c)
        return rcopy(qall.at[c, m2], qall.at[c, m2], a2s.at[c, h], a2r.at[c, h], peer(near[h]))

    def ag2f(c, h):
        _, (m2, peer) = axes(c)
        a = (m2 + side - near[h]) % side
        return rcopy(qall.at[c, a, part(h)], qall.at[c, a, part(h)], a2s.at[c, 2 + h], a2r.at[c, 2 + h], peer(near[h]))

    def ag3(c, d):
        _, (m2, _) = axes(c)
        a = (m2 + side - d) % side
        return rcopy(qall.at[c, a], qall.at[c, side + a], a3s.at[c, d], a3r.at[c, d], sib)

    def od(c):
        return rcopy(osend.at[c % NSLOT], orecv.at[c], ods.at[c], odr.at[c], sib)

    def rs1(c, h):
        _, (m2, peer) = axes(c)
        return rcopy(p1s.at[c, (m2 + near[h]) % side], p1r.at[c, m2], s1.at[c, h], r1.at[c, h], peer(near[h]))

    def rs1x(c, h):
        _, (m2, peer) = axes(c)
        return rcopy(p1s.at[c, (m2 + 2) % side, part(h)], p1x.at[c, h], s1.at[c, 2 + h], r1.at[c, 2 + h], peer(near[h]))

    def rs1f(c, h):
        _, (m2, peer) = axes(c)
        a = (m2 + side - near[h]) % side
        return rcopy(p1x.at[c, h], p1r.at[c, a, part(h)], s1.at[c, 4 + h], r1.at[c, 4 + h], peer(near[h]))

    def rl1(c, d):
        _, (m2, peer) = axes(c)
        return rcopy(l1s.at[c], l1r.at[c, m2], sl1.at[c, d - 1], rr1.at[c, d - 1], peer(d))

    def rs2(c, h):
        (m1, peer), _ = axes(c)
        return rcopy(p2s.at[c, (m1 + near[h]) % side], p2r.at[c, m1], s2.at[c, h], r2.at[c, h], peer(near[h]))

    def rs2x(c, h):
        (m1, peer), _ = axes(c)
        return rcopy(p2s.at[c, (m1 + 2) % side, part(h)], p2x.at[c, h], s2.at[c, 2 + h], r2.at[c, 2 + h], peer(near[h]))

    def rs2f(c, h):
        (m1, peer), _ = axes(c)
        a = (m1 + side - near[h]) % side
        return rcopy(p2x.at[c, h], p2r.at[c, a, part(h)], s2.at[c, 4 + h], r2.at[c, 4 + h], peer(near[h]))

    def rl2(c, d):
        (m1, peer), _ = axes(c)
        return rcopy(l2s.at[c], l2r.at[c, m1], sl2.at[c, d - 1], rr2.at[c, d - 1], peer(d))

    def cload(b):
        return pltpu.make_async_copy(cache_ref.at[b], cbuf.at[b % NBUF], csem.at[b % NBUF])

    for b in range(min(NBUF, total)):
        cload(b).start()

    barrier = pltpu.get_barrier_semaphore()
    peers = [sib] + [at(y, (x + d) % side, core) for d in dists] + [at((y + d) % side, x, core) for d in dists]
    for dev in peers:
        pl.semaphore_signal(barrier, inc=1, device_id=dev, device_id_type=pl.DeviceIdType.MESH)
    pl.semaphore_wait(barrier, len(peers))

    def gather_start(c):
        for h in range(2):
            ag1(c, h).start()

    def gather_relay(c):
        for h in range(2):
            ag1(c, h).wait_recv()
            ag1f(c, h).start()

    def gather_first(c):
        (m1, _), (m2, _) = axes(c)
        g1[c, m1] = q_ref[pl.ds(c * nb, nb)]
        for h in range(2):
            ag1f(c, h).wait_recv()

        def body(i, _):
            parts = [g1[c, a, i].astype(jnp.float32) for a in range(side)]
            qall[c, m2, i] = jnp.concatenate(parts, axis=0).astype(qall.dtype)
            return 0

        lax.fori_loop(0, nb, body, 0)
        for h in range(2):
            ag2(c, h).start()
        ag3(c, 0).start()

    def gather_second(c):
        for h in range(2):
            ag2(c, h).wait_recv()
            ag2f(c, h).start()
            ag3(c, near[h]).start()

    def gather_far(c):
        for h in range(2):
            ag2f(c, h).wait_recv()
        ag3(c, 2).start()

    def gather_third(c):
        for d in range(side):
            ag3(c, d).wait_recv()

    tpos = lax.broadcasted_iota(jnp.int32, (1, t), 1)
    pos = (tpos // page) * (page * n) + me * page + tpos % page

    def scores(b, ref):
        ref[...] = lax.dot_general(qall[b // nb, :, b % nb].reshape(2 * half, k), cbuf[b % NBUF],
                                   (((1,), (1,)), ((), ())), preferred_element_type=jnp.float32)

    def attend(c, i, ref):
        b = c * nb + i
        s = jnp.where(pos < lens_ref[b], ref[...], NEG)
        m = jnp.max(s, axis=1, keepdims=True)
        ms = jnp.where(m == NEG, 0.0, m)
        p = jnp.exp((s - ms) * SCALE)
        l = jnp.sum(p, axis=1, keepdims=True)
        acc = lax.dot_general(p.astype(jnp.bfloat16), cbuf[b % NBUF, :, :lorav], (((1,), (0,)), ((), ())),
                              preferred_element_type=jnp.float32)
        ls = jnp.where(l > 0.0, l, 1.0)
        o = acc * (1.0 / ls)
        lse = jnp.broadcast_to(jnp.where(l > 0.0, ms * SCALE + jnp.log(ls), NEG), (2 * half, LANES))
        own[c % NSLOT, i, :, :lorav] = o[:half]
        own[c % NSLOT, i, :, lorav:] = lse[:half]
        osend[c % NSLOT, i, :, :lorav] = o[half:]
        osend[c % NSLOT, i, :, lorav:] = lse[half:]

    def compute(c):
        @pl.when(c >= NSLOT)
        def _():
            od(c - NSLOT).wait_send()

        @pl.when(c == 0)
        def _():
            cload(0).wait()
            scores(0, sb0)

        def two(j, _):
            b = c * nb + 2 * j
            cload(b + 1).wait()

            @pl.when(b + 2 < total)
            def _():
                cload(b + 2).wait()

            scores(b + 1, sb1)
            attend(c, 2 * j, sb0)
            scores(jnp.minimum(b + 2, total - 1), sb0)
            attend(c, 2 * j + 1, sb1)
            for later in range(NBUF, NBUF + 2):
                @pl.when(b + later < total)
                def _():
                    cload(b + later).start()

            return 0

        lax.fori_loop(0, nb // 2, two, 0)
        od(c).start()

    diag = lax.broadcasted_iota(jnp.int32, (half, LANES), 0) == lax.broadcasted_iota(jnp.int32, (half, LANES), 1)

    def pair(c):
        od(c).wait_recv()

        def one(i, _):
            la = own[c % NSLOT, i, :, lorav:]
            lb = orecv[c, i, :, lorav:]
            top = jnp.maximum(la, lb)
            ts = jnp.where(top == NEG, 0.0, top)
            wa = jnp.exp(la - ts)
            wb = jnp.exp(lb - ts)
            ws = wa + wb
            wss = jnp.where(ws > 0.0, ws, 1.0)
            inv = 1.0 / wss
            wa = wa * inv
            wb = wb * inv
            for j in range(lorav // LANES):
                cols = slice(j * LANES, (j + 1) * LANES)
                v = (wa * own[c % NSLOT, i, :, cols] + wb * orecv[c, i, :, cols]).astype(jnp.bfloat16)
                p1s[c, :, i, :, cols] = v.reshape(side, tile, LANES)
            lse = jnp.where(ws > 0.0, ts + jnp.log(wss), NEG)
            l1s[c, pl.ds(i, 1)] = jnp.sum(jnp.where(diag, lse, 0.0), axis=0, keepdims=True)
            return 0

        lax.fori_loop(0, nb, one, 0)
        for h in range(2):
            rs1x(c, h).start()
        for d in dists:
            rl1(c, d).start()
        for h in range(2):
            rs1(c, h).start()

    def pair_relay(c):
        for h in range(2):
            rs1x(c, h).wait_recv()
            rs1f(c, h).start()

    def weights(ls):
        top = functools.reduce(jnp.maximum, ls)
        ts = jnp.where(top == NEG, 0.0, top)
        w = [jnp.exp(v - ts) for v in ls]
        ws = functools.reduce(jnp.add, w)
        wss = jnp.where(ws > 0.0, ws, 1.0)
        inv = 1.0 / wss
        for j, v in enumerate(w):
            wrow[j] = v * inv
        return jnp.where(ws > 0.0, ts + jnp.log(wss), NEG)

    def combine(i, rows, first, srcs):
        sel = (lax.broadcasted_iota(jnp.int32, (rows, LANES), 0) + first
               == lax.broadcasted_iota(jnp.int32, (rows, LANES), 1))
        tot = None
        for j, src in enumerate(srcs):
            w = jnp.broadcast_to(wrow[j, pl.ds(i, 1)], (rows, LANES))
            w = jnp.sum(jnp.where(sel, w, 0.0), axis=1, keepdims=True)
            term = w * src[i].astype(jnp.float32)
            tot = term if tot is None else tot + term
        return tot

    def second(c):
        (m1, _), (m2, _) = axes(c)
        for h in range(2):
            rs1(c, h).wait_recv()
            rs1f(c, h).wait_recv()
        for d in dists:
            rl1(c, d).wait_recv()
        idx = [(m2 + d) % side for d in dists]
        l2s[c] = weights([l1s[c]] + [l1r[c, a] for a in idx])
        srcs = [p1s.at[c, m2]] + [p1r.at[c, a] for a in idx]

        def one(i, _):
            v = combine(i, tile, m2 * tile, srcs)
            for a in range(side):
                p2s[c, a, i] = v[a * hl:(a + 1) * hl]
            return 0

        lax.fori_loop(0, nb, one, 0)
        for h in range(2):
            rs2x(c, h).start()
        for d in dists:
            rl2(c, d).start()
        for h in range(2):
            rs2(c, h).start()

    def second_relay(c):
        for h in range(2):
            rs2x(c, h).wait_recv()
            rs2f(c, h).start()

    def final(c):
        (m1, _), (m2, _) = axes(c)
        for h in range(2):
            rs2(c, h).wait_recv()
            rs2f(c, h).wait_recv()
        for d in dists:
            rl2(c, d).wait_recv()
        idx = [(m1 + d) % side for d in dists]
        weights([l2s[c]] + [l2r[c, a] for a in idx])
        srcs = [p2s.at[c, m1]] + [p2r.at[c, a] for a in idx]

        def one(i, _):
            out_ref[c * nb + i] = combine(i, hl, m2 * tile + m1 * hl, srcs).astype(out_ref.dtype)
            return 0

        lax.fori_loop(0, nb, one, 0)

    def each(stage):
        def one(c, _):
            stage(c)
            return 0

        lax.fori_loop(0, nc, one, 0)

    each(gather_start)
    each(gather_relay)

    stages = ((gather_first, 0), (gather_second, 6), (gather_far, 12), (gather_third, 13), (compute, 14), (pair, 16),
              (pair_relay, 19), (second, 22), (second_relay, 26), (final, 30))

    def step(i, _):
        for stage, delay in stages:
            @pl.when((i >= delay) & (i < delay + nc))
            def _():
                stage(jnp.maximum(i - delay, 0))

        return 0

    lax.fori_loop(0, nc + stages[-1][1], step, 0)

    def drain(c):
        for h in range(2):
            for cp in (ag1, ag1f, ag2, ag2f, rs1, rs1x, rs1f, rs2, rs2x, rs2f):
                cp(c, h).wait_send()
        for d in dists:
            rl1(c, d).wait_send()
            rl2(c, d).wait_send()
        for d in range(side):
            ag3(c, d).wait_send()

        @pl.when(c >= nc - NSLOT)
        def _():
            od(c).wait_send()

    each(drain)


def solution(mesh):
    n = mesh.shape['dcp']
    side = math.isqrt(n // 2)

    def local(q, cache, lens):
        b, hl, k = q.shape
        t = cache.shape[1] * cache.shape[3]
        lorav = k - ROPE
        nb = min(4, max(1, b // 2))
        nc = b // nb
        tile = side * hl
        half = side * tile
        bf, f32 = jnp.bfloat16, jnp.float32
        dma = pltpu.SemaphoreType.DMA
        return pl.pallas_call(
            functools.partial(kernel, n, side, nc, nb, cache.shape[3]),
            out_shape=jax.ShapeDtypeStruct((b, hl, lorav), bf),
            in_specs=[pl.BlockSpec(memory_space=pltpu.VMEM), pl.BlockSpec(memory_space=pl.ANY),
                      pl.BlockSpec(memory_space=pltpu.SMEM)],
            out_specs=pl.BlockSpec(memory_space=pltpu.VMEM),
            scratch_shapes=[
                pltpu.VMEM((nc, side, nb, hl, k), bf),
                pltpu.VMEM((nc, 2 * side, nb, tile, k), bf),
                pltpu.VMEM((NBUF, t, k), bf),
                pltpu.VMEM((NSLOT, nb, half, lorav + LANES), f32),
                pltpu.VMEM((NSLOT, nb, half, lorav + LANES), f32),
                pltpu.VMEM((nc, nb, half, lorav + LANES), f32),
                pltpu.VMEM((nc, side, nb, tile, lorav), bf),
                pltpu.VMEM((nc, 2, nb // 2, tile, lorav), bf),
                pltpu.VMEM((nc, side, nb, tile, lorav), bf),
                pltpu.VMEM((nc, nb, LANES), f32),
                pltpu.VMEM((nc, side, nb, LANES), f32),
                pltpu.VMEM((nc, side, nb, hl, lorav), f32),
                pltpu.VMEM((nc, 2, nb // 2, hl, lorav), f32),
                pltpu.VMEM((nc, side, nb, hl, lorav), f32),
                pltpu.VMEM((nc, nb, LANES), f32),
                pltpu.VMEM((nc, side, nb, LANES), f32),
                pltpu.VMEM((side, nb, LANES), f32),
                pltpu.VMEM((2 * half, t), f32), pltpu.VMEM((2 * half, t), f32),
                dma((NBUF,)),
                dma((nc, 4)), dma((nc, 4)), dma((nc, 4)), dma((nc, 4)),
                dma((nc, side)), dma((nc, side)),
                dma((nc,)), dma((nc,)),
                dma((nc, 6)), dma((nc, 6)), dma((nc, side - 1)), dma((nc, side - 1)),
                dma((nc, 6)), dma((nc, 6)), dma((nc, side - 1)), dma((nc, side - 1)),
            ],
            compiler_params=pltpu.CompilerParams(collective_id=0, has_side_effects=True,
                                                 vmem_limit_bytes=63 * 1024 * 1024),
        )(q, cache.reshape(b, t, k), lens)

    return jax.shard_map(local, mesh=mesh, in_specs=(P('dp', 'dcp', None), P('dp', None, 'dcp', None, None), P('dp')),
                         out_specs=P('dp', 'dcp', None), check_vma=False)
```

```python
import functools
import math

import jax
import jax.numpy as jnp
from jax import lax
from jax.experimental import pallas as pl
from jax.experimental.pallas import tpu as pltpu
from jax.sharding import PartitionSpec as P

ROPE = 64
QK_DIM = 192
SCALE = QK_DIM ** -0.5
NEG = float('-inf')
LANES = 128
NBUF = 6
NSLOT = 4


def kernel(n, side, nc, nb, page, q_ref, cache_ref, lens_ref, out_ref,
           g1, qall, cbuf, own, osend, orecv, p1s, p1x, p1r, l1s, l1r, p2s, p2x, p2r, l2s, l2r, wrow, sb0, sb1,
           csem, a1s, a1r, a2s, a2r, a3s, a3r, ods, odr, s1, r1, sl1, rr1, s2, r2, sl2, rr2):
    hl = q_ref.shape[1]
    k = q_ref.shape[2]
    t = cbuf.shape[1]
    lorav = k - ROPE
    tile = side * hl
    half = side * tile
    total = nc * nb
    each_type = total // 2

    def row(c):
        return (c // 2) * nb

    def seq(b):
        c = b // nb
        return (c % 2) * each_type + row(c) + b % nb

    me = lax.axis_index('dcp')
    core = me % 2
    x = (me // 2) % side
    y = me // (2 * side)
    dists = tuple(range(1, side))

    def at(yy, xx, cc):
        return {'dcp': (yy * side + xx) * 2 + cc}

    sib = at(y, x, 1 - core)

    def axes(c):
        odd = c % 2
        return ((x + odd * (y - x), lambda d: at((y + odd * d) % side, (x + (1 - odd) * d) % side, core)),
                (y + odd * (x - y), lambda d: at((y + (1 - odd) * d) % side, (x + odd * d) % side, core)))

    def rcopy(src, dst, ss, rs, dev):
        return pltpu.make_async_remote_copy(src_ref=src, dst_ref=dst, send_sem=ss, recv_sem=rs, device_id=dev,
                                            device_id_type=pl.DeviceIdType.MESH)

    hb = nb // 2

    def part(h):
        return pl.ds(h * hb, hb)

    near = (1, side - 1)

    bounds = [0, min(2 * nb, each_type), each_type]
    pieces = [p for p in range(len(bounds) - 1) if bounds[p + 1] > bounds[p]]

    def ag1(p, ty, h):
        (m1, peer), _ = axes(ty)
        at_ = pl.ds(bounds[p], bounds[p + 1] - bounds[p])
        return rcopy(q_ref.at[pl.ds(ty * each_type + bounds[p], bounds[p + 1] - bounds[p])], g1.at[ty, m1, at_],
                     a1s.at[p, ty, h], a1r.at[p, ty, h], peer(near[h]))

    def ag1f(p, ty, h):
        (m1, peer), _ = axes(ty)
        a = (m1 + side - near[h]) % side
        size = (bounds[p + 1] - bounds[p]) // 2
        at_ = pl.ds(bounds[p] + h * size, size)
        return rcopy(g1.at[ty, a, at_], g1.at[ty, a, at_], a1s.at[p, ty, 2 + h], a1r.at[p, ty, 2 + h], peer(near[h]))

    def ag2(c, h):
        _, (m2, peer) = axes(c)
        return rcopy(qall.at[c, m2], qall.at[c, m2], a2s.at[c, h], a2r.at[c, h], peer(near[h]))

    def ag2f(c, h):
        _, (m2, peer) = axes(c)
        a = (m2 + side - near[h]) % side
        return rcopy(qall.at[c, a, part(h)], qall.at[c, a, part(h)], a2s.at[c, 2 + h], a2r.at[c, 2 + h], peer(near[h]))

    def ag3(c, d):
        _, (m2, _) = axes(c)
        a = (m2 + side - d) % side
        return rcopy(qall.at[c, a], qall.at[c, side + a], a3s.at[c, d], a3r.at[c, d], sib)

    def od(c):
        return rcopy(osend.at[c % NSLOT], orecv.at[c], ods.at[c], odr.at[c], sib)

    def rs1(c, h):
        _, (m2, peer) = axes(c)
        return rcopy(p1s.at[c, (m2 + near[h]) % side], p1r.at[c, m2], s1.at[c, h], r1.at[c, h], peer(near[h]))

    def rs1x(c, h):
        _, (m2, peer) = axes(c)
        return rcopy(p1s.at[c, (m2 + 2) % side, part(h)], p1x.at[c, h], s1.at[c, 2 + h], r1.at[c, 2 + h], peer(near[h]))

    def rs1f(c, h):
        _, (m2, peer) = axes(c)
        a = (m2 + side - near[h]) % side
        return rcopy(p1x.at[c, h], p1r.at[c, a, part(h)], s1.at[c, 4 + h], r1.at[c, 4 + h], peer(near[h]))

    def both(c):
        return pl.ds((c // 4) * 2, 2)

    def rl1(c, d):
        _, (m2, peer) = axes(c)
        return rcopy(l1s.at[c % 2, both(c)], l1r.at[c % 2, m2, both(c)], sl1.at[c % 2, c // 4, d - 1],
                     rr1.at[c % 2, c // 4, d - 1], peer(d))

    def rs2(c, h):
        (m1, peer), _ = axes(c)
        return rcopy(p2s.at[c, (m1 + near[h]) % side], p2r.at[c, m1], s2.at[c, h], r2.at[c, h], peer(near[h]))

    def rs2x(c, h):
        (m1, peer), _ = axes(c)
        return rcopy(p2s.at[c, (m1 + 2) % side, part(h)], p2x.at[c, h], s2.at[c, 2 + h], r2.at[c, 2 + h], peer(near[h]))

    def rs2f(c, h):
        (m1, peer), _ = axes(c)
        a = (m1 + side - near[h]) % side
        return rcopy(p2x.at[c, h], p2r.at[c, a, part(h)], s2.at[c, 4 + h], r2.at[c, 4 + h], peer(near[h]))

    def rl2(c, d):
        (m1, peer), _ = axes(c)
        return rcopy(l2s.at[c % 2, both(c)], l2r.at[c % 2, m1, both(c)], sl2.at[c % 2, c // 4, d - 1],
                     rr2.at[c % 2, c // 4, d - 1], peer(d))

    def cload(b):
        return pltpu.make_async_copy(cache_ref.at[seq(b)], cbuf.at[b % NBUF], csem.at[b % NBUF])

    for b in range(min(NBUF, total)):
        cload(b).start()

    barrier = pltpu.get_barrier_semaphore()
    peers = [sib] + [at(y, (x + d) % side, core) for d in dists] + [at((y + d) % side, x, core) for d in dists]
    for dev in peers:
        pl.semaphore_signal(barrier, inc=1, device_id=dev, device_id_type=pl.DeviceIdType.MESH)
    pl.semaphore_wait(barrier, len(peers))

    def gather_far_rows(p):
        for ty in range(2):
            for h in range(2):
                ag1f(p, ty, h).wait_recv()

    for p in pieces:
        for ty in range(2):
            for h in range(2):
                ag1(p, ty, h).start()
    for p in pieces:
        for ty in range(2):
            (m1, _), _ = axes(ty)
            g1[ty, m1, bounds[p]:bounds[p + 1]] = q_ref[ty * each_type + bounds[p]:ty * each_type + bounds[p + 1]]
            for h in range(2):
                ag1(p, ty, h).wait_recv()
                ag1f(p, ty, h).start()
    gather_far_rows(0)

    def gather_first(c):
        _, (m2, _) = axes(c)
        if len(pieces) > 1:
            @pl.when(c == 2 * bounds[1] // nb)
            def _():
                gather_far_rows(1)

        def body(i, _):
            parts = [g1[c % 2, a, row(c) + i].astype(jnp.float32) for a in range(side)]
            qall[c, m2, i] = jnp.concatenate(parts, axis=0).astype(qall.dtype)
            return 0

        lax.fori_loop(0, nb, body, 0)
        for h in range(2):
            ag2(c, h).start()
        ag3(c, 0).start()

    def gather_second(c):
        for h in range(2):
            ag2(c, h).wait_recv()
            ag2f(c, h).start()
            ag3(c, near[h]).start()

    def gather_far(c):
        for h in range(2):
            ag2f(c, h).wait_recv()
        ag3(c, 2).start()

    def gather_third(c):
        for d in range(side):
            ag3(c, d).wait_recv()

    tpos = lax.broadcasted_iota(jnp.int32, (1, t), 1)
    pos = (tpos // page) * (page * n) + me * page + tpos % page

    def scores(b, ref):
        ref[...] = lax.dot_general(qall[b // nb, :, b % nb].reshape(2 * half, k), cbuf[b % NBUF],
                                   (((1,), (1,)), ((), ())), preferred_element_type=jnp.float32)

    def attend(c, i, ref):
        b = c * nb + i
        s = jnp.where(pos < lens_ref[seq(b)], ref[...], NEG)
        m = jnp.max(s, axis=1, keepdims=True)
        ms = jnp.where(m == NEG, 0.0, m)
        p = jnp.exp((s - ms) * SCALE)
        l = jnp.sum(p, axis=1, keepdims=True)
        acc = lax.dot_general(p.astype(jnp.bfloat16), cbuf[b % NBUF, :, :lorav], (((1,), (0,)), ((), ())),
                              preferred_element_type=jnp.float32)
        ls = jnp.where(l > 0.0, l, 1.0)
        o = acc * (1.0 / ls)
        lse = jnp.broadcast_to(jnp.where(l > 0.0, ms * SCALE + jnp.log(ls), NEG), (2 * half, LANES))
        own[c % NSLOT, i, :, :lorav] = o[:half]
        own[c % NSLOT, i, :, lorav:] = lse[:half]
        osend[c % NSLOT, i, :, :lorav] = o[half:]
        osend[c % NSLOT, i, :, lorav:] = lse[half:]

    def compute(c):
        @pl.when(c >= NSLOT)
        def _():
            od(c - NSLOT).wait_send()

        @pl.when(c == 0)
        def _():
            cload(0).wait()
            scores(0, sb0)

        def two(j, _):
            b = c * nb + 2 * j
            cload(b + 1).wait()

            @pl.when(b + 2 < total)
            def _():
                cload(b + 2).wait()

            scores(b + 1, sb1)
            attend(c, 2 * j, sb0)
            scores(jnp.minimum(b + 2, total - 1), sb0)
            attend(c, 2 * j + 1, sb1)
            for later in range(NBUF, NBUF + 2):
                @pl.when(b + later < total)
                def _():
                    cload(b + later).start()

            return 0

        lax.fori_loop(0, nb // 2, two, 0)
        od(c).start()

    diag = lax.broadcasted_iota(jnp.int32, (half, LANES), 0) == lax.broadcasted_iota(jnp.int32, (half, LANES), 1)

    def pair(c):
        od(c).wait_recv()

        def one(i, _):
            la = own[c % NSLOT, i, :, lorav:]
            lb = orecv[c, i, :, lorav:]
            top = jnp.maximum(la, lb)
            ts = jnp.where(top == NEG, 0.0, top)
            wa = jnp.exp(la - ts)
            wb = jnp.exp(lb - ts)
            ws = wa + wb
            wss = jnp.where(ws > 0.0, ws, 1.0)
            inv = 1.0 / wss
            wa = wa * inv
            wb = wb * inv
            for j in range(lorav // LANES):
                cols = slice(j * LANES, (j + 1) * LANES)
                v = (wa * own[c % NSLOT, i, :, cols] + wb * orecv[c, i, :, cols]).astype(jnp.bfloat16)
                p1s[c, :, i, :, cols] = v.reshape(side, tile, LANES)
            lse = jnp.where(ws > 0.0, ts + jnp.log(wss), NEG)
            l1s[c % 2, c // 2, pl.ds(i, 1)] = jnp.sum(jnp.where(diag, lse, 0.0), axis=0, keepdims=True)
            return 0

        lax.fori_loop(0, nb, one, 0)
        for h in range(2):
            rs1x(c, h).start()

        @pl.when((c // 2) % 2 == 1)
        def _():
            for d in dists:
                rl1(c, d).start()

        for h in range(2):
            rs1(c, h).start()

    def pair_relay(c):
        for h in range(2):
            rs1x(c, h).wait_recv()
            rs1f(c, h).start()

    def weights(ls):
        top = functools.reduce(jnp.maximum, ls)
        ts = jnp.where(top == NEG, 0.0, top)
        w = [jnp.exp(v - ts) for v in ls]
        ws = functools.reduce(jnp.add, w)
        wss = jnp.where(ws > 0.0, ws, 1.0)
        inv = 1.0 / wss
        for j, v in enumerate(w):
            wrow[j] = v * inv
        return jnp.where(ws > 0.0, ts + jnp.log(wss), NEG)

    def combine(i, rows, first, srcs):
        sel = (lax.broadcasted_iota(jnp.int32, (rows, LANES), 0) + first
               == lax.broadcasted_iota(jnp.int32, (rows, LANES), 1))
        tot = None
        for j, src in enumerate(srcs):
            w = jnp.broadcast_to(wrow[j, pl.ds(i, 1)], (rows, LANES))
            w = jnp.sum(jnp.where(sel, w, 0.0), axis=1, keepdims=True)
            term = w * src[i].astype(jnp.float32)
            tot = term if tot is None else tot + term
        return tot

    def second(c):
        (m1, _), (m2, _) = axes(c)
        for h in range(2):
            rs1(c, h).wait_recv()
            rs1f(c, h).wait_recv()

        @pl.when((c // 2) % 2 == 0)
        def _():
            for d in dists:
                rl1(c, d).wait_recv()

        idx = [(m2 + d) % side for d in dists]
        l2s[c % 2, c // 2] = weights([l1s[c % 2, c // 2]] + [l1r[c % 2, a, c // 2] for a in idx])
        srcs = [p1s.at[c, m2]] + [p1r.at[c, a] for a in idx]

        def one(i, _):
            v = combine(i, tile, m2 * tile, srcs)
            for a in range(side):
                p2s[c, a, i] = v[a * hl:(a + 1) * hl]
            return 0

        lax.fori_loop(0, nb, one, 0)
        for h in range(2):
            rs2x(c, h).start()

        @pl.when((c // 2) % 2 == 1)
        def _():
            for d in dists:
                rl2(c, d).start()

        for h in range(2):
            rs2(c, h).start()

    def second_relay(c):
        for h in range(2):
            rs2x(c, h).wait_recv()
            rs2f(c, h).start()

    def final(c):
        (m1, _), (m2, _) = axes(c)
        for h in range(2):
            rs2(c, h).wait_recv()
            rs2f(c, h).wait_recv()

        @pl.when((c // 2) % 2 == 0)
        def _():
            for d in dists:
                rl2(c, d).wait_recv()

        idx = [(m1 + d) % side for d in dists]
        weights([l2s[c % 2, c // 2]] + [l2r[c % 2, a, c // 2] for a in idx])
        srcs = [p2s.at[c, m1]] + [p2r.at[c, a] for a in idx]

        def one(i, _):
            out_ref[seq(c * nb + i)] = combine(i, hl, m2 * tile + m1 * hl, srcs).astype(out_ref.dtype)
            return 0

        lax.fori_loop(0, nb, one, 0)

    def each(stage):
        def one(c, _):
            stage(c)
            return 0

        lax.fori_loop(0, nc, one, 0)

    stages = ((gather_third, 10), (gather_first, 0), (compute, 11), (gather_second, 5), (pair_relay, 14),
              (second_relay, 27), (gather_far, 8), (final, 38), (second, 18), (pair, 12))

    def step(i, _):
        for stage, delay in stages:
            @pl.when((i >= delay) & (i < delay + nc))
            def _():
                stage(jnp.maximum(i - delay, 0))

        return 0

    lax.fori_loop(0, nc + max(d for _, d in stages), step, 0)

    def drain(c):
        for h in range(2):
            for cp in (ag2, ag2f, rs1, rs1x, rs1f, rs2, rs2x, rs2f):
                cp(c, h).wait_send()

        @pl.when((c // 2) % 2 == 1)
        def _():
            for d in dists:
                rl1(c, d).wait_send()
                rl2(c, d).wait_send()

        for d in range(side):
            ag3(c, d).wait_send()

        @pl.when(c >= nc - NSLOT)
        def _():
            od(c).wait_send()

    each(drain)
    for p in pieces:
        for ty in range(2):
            for h in range(2):
                ag1(p, ty, h).wait_send()
                ag1f(p, ty, h).wait_send()


def solution(mesh):
    n = mesh.shape['dcp']
    side = math.isqrt(n // 2)

    def local(q, cache, lens):
        b, hl, k = q.shape
        t = cache.shape[1] * cache.shape[3]
        lorav = k - ROPE
        nb = min(4, max(1, b // 4))
        nc = b // nb
        tile = side * hl
        half = side * tile
        bf, f32 = jnp.bfloat16, jnp.float32
        dma = pltpu.SemaphoreType.DMA
        return pl.pallas_call(
            functools.partial(kernel, n, side, nc, nb, cache.shape[3]),
            out_shape=jax.ShapeDtypeStruct((b, hl, lorav), bf),
            in_specs=[pl.BlockSpec(memory_space=pltpu.VMEM), pl.BlockSpec(memory_space=pl.ANY),
                      pl.BlockSpec(memory_space=pltpu.SMEM)],
            out_specs=pl.BlockSpec(memory_space=pltpu.VMEM),
            scratch_shapes=[
                pltpu.VMEM((2, side, b // 2, hl, k), bf),
                pltpu.VMEM((nc, 2 * side, nb, tile, k), bf),
                pltpu.VMEM((NBUF, t, k), bf),
                pltpu.VMEM((NSLOT, nb, half, lorav + LANES), f32),
                pltpu.VMEM((NSLOT, nb, half, lorav + LANES), f32),
                pltpu.VMEM((nc, nb, half, lorav + LANES), f32),
                pltpu.VMEM((nc, side, nb, tile, lorav), bf),
                pltpu.VMEM((nc, 2, nb // 2, tile, lorav), bf),
                pltpu.VMEM((nc, side, nb, tile, lorav), bf),
                pltpu.VMEM((2, nc // 2, nb, LANES), f32),
                pltpu.VMEM((2, side, nc // 2, nb, LANES), f32),
                pltpu.VMEM((nc, side, nb, hl, lorav), f32),
                pltpu.VMEM((nc, 2, nb // 2, hl, lorav), f32),
                pltpu.VMEM((nc, side, nb, hl, lorav), f32),
                pltpu.VMEM((2, nc // 2, nb, LANES), f32),
                pltpu.VMEM((2, side, nc // 2, nb, LANES), f32),
                pltpu.VMEM((side, nb, LANES), f32),
                pltpu.VMEM((2 * half, t), f32), pltpu.VMEM((2 * half, t), f32),
                dma((NBUF,)),
                dma((2, 2, 4)), dma((2, 2, 4)), dma((nc, 4)), dma((nc, 4)),
                dma((nc, side)), dma((nc, side)),
                dma((nc,)), dma((nc,)),
                dma((nc, 6)), dma((nc, 6)), dma((2, nc // 4, side - 1)), dma((2, nc // 4, side - 1)),
                dma((nc, 6)), dma((nc, 6)), dma((2, nc // 4, side - 1)), dma((2, nc // 4, side - 1)),
            ],
            compiler_params=pltpu.CompilerParams(collective_id=0, has_side_effects=True,
                                                 vmem_limit_bytes=63 * 1024 * 1024),
        )(q, cache.reshape(b, t, k), lens)

    return jax.shard_map(local, mesh=mesh, in_specs=(P('dp', 'dcp', None), P('dp', None, 'dcp', None, None), P('dp')),
                         out_specs=P('dp', 'dcp', None), check_vma=False)
```

```python
import functools
import math

import jax
import jax.numpy as jnp
from jax import lax
from jax.experimental import pallas as pl
from jax.experimental.pallas import tpu as pltpu
from jax.sharding import PartitionSpec as P

ROPE = 64
QK_DIM = 192
SCALE = QK_DIM ** -0.5
NEG = float('-inf')
LANES = 128
NBUF = 6
NSLOT = 4
LAG = 2


def kernel(n, side, nc, nb, page, q_ref, cache_ref, lens_ref, out_ref,
           g1, qall, cbuf, own, osend, orecv, p1s, p1x, p1r, l1s, l1r, p2s, p2x, p2r, l2s, l2r, wrow, sb0, sb1,
           csem, a1s, a1r, a2s, a2r, a3s, a3r, ods, odr, s1, r1, sl1, rr1, s2, r2, sl2, rr2):
    hl = q_ref.shape[1]
    k = q_ref.shape[2]
    t = cbuf.shape[1]
    lorav = k - ROPE
    tile = side * hl
    half = side * tile
    total = nc * nb
    each_type = total // 2

    def row(c):
        return (c // 2) * nb

    def seq(b):
        c = b // nb
        return (c % 2) * each_type + row(c) + b % nb

    me = lax.axis_index('dcp')
    core = me % 2
    x = (me // 2) % side
    y = me // (2 * side)
    dists = tuple(range(1, side))

    def at(yy, xx, cc):
        return {'dcp': (yy * side + xx) * 2 + cc}

    sib = at(y, x, 1 - core)

    def axes(c):
        odd = c % 2
        return ((x + odd * (y - x), lambda d: at((y + odd * d) % side, (x + (1 - odd) * d) % side, core)),
                (y + odd * (x - y), lambda d: at((y + (1 - odd) * d) % side, (x + odd * d) % side, core)))

    def rcopy(src, dst, ss, rs, dev):
        return pltpu.make_async_remote_copy(src_ref=src, dst_ref=dst, send_sem=ss, recv_sem=rs, device_id=dev,
                                            device_id_type=pl.DeviceIdType.MESH)

    hb = nb // 2

    def part(h):
        return pl.ds(h * hb, hb)

    near = (1, side - 1)

    bounds = [0, min(2 * nb, each_type), each_type]
    pieces = [p for p in range(len(bounds) - 1) if bounds[p + 1] > bounds[p]]

    def ag1(p, ty, h):
        (m1, peer), _ = axes(ty)
        at_ = pl.ds(bounds[p], bounds[p + 1] - bounds[p])
        return rcopy(q_ref.at[pl.ds(ty * each_type + bounds[p], bounds[p + 1] - bounds[p])], g1.at[ty, m1, at_],
                     a1s.at[p, ty, h], a1r.at[p, ty, h], peer(near[h]))

    def ag1f(p, ty, h):
        (m1, peer), _ = axes(ty)
        a = (m1 + side - near[h]) % side
        size = (bounds[p + 1] - bounds[p]) // 2
        at_ = pl.ds(bounds[p] + h * size, size)
        return rcopy(g1.at[ty, a, at_], g1.at[ty, a, at_], a1s.at[p, ty, 2 + h], a1r.at[p, ty, 2 + h], peer(near[h]))

    def ag2(c, h):
        _, (m2, peer) = axes(c)
        return rcopy(qall.at[c, m2], qall.at[c, m2], a2s.at[c, h], a2r.at[c, h], peer(near[h]))

    def ag2f(c, h):
        _, (m2, peer) = axes(c)
        a = (m2 + side - near[h]) % side
        return rcopy(qall.at[c, a, part(h)], qall.at[c, a, part(h)], a2s.at[c, 2 + h], a2r.at[c, 2 + h], peer(near[h]))

    def ag3(c, d):
        _, (m2, _) = axes(c)
        a = (m2 + side - d) % side
        return rcopy(qall.at[c, a], qall.at[c, side + a], a3s.at[c, d], a3r.at[c, d], sib)

    def od(c):
        return rcopy(osend.at[c % NSLOT], orecv.at[c], ods.at[c], odr.at[c], sib)

    def rs1(c, h):
        _, (m2, peer) = axes(c)
        return rcopy(p1s.at[c, (m2 + near[h]) % side], p1r.at[c, m2], s1.at[c, h], r1.at[c, h], peer(near[h]))

    def rs1x(c, h):
        _, (m2, peer) = axes(c)
        return rcopy(p1s.at[c, (m2 + 2) % side, part(h)], p1x.at[c, h], s1.at[c, 2 + h], r1.at[c, 2 + h], peer(near[h]))

    def rs1f(c, h):
        _, (m2, peer) = axes(c)
        a = (m2 + side - near[h]) % side
        return rcopy(p1x.at[c, h], p1r.at[c, a, part(h)], s1.at[c, 4 + h], r1.at[c, 4 + h], peer(near[h]))

    def both(c):
        return pl.ds((c // 4) * 2, 2)

    def rl1(c, d):
        _, (m2, peer) = axes(c)
        return rcopy(l1s.at[c % 2, both(c)], l1r.at[c % 2, m2, both(c)], sl1.at[c % 2, c // 4, d - 1],
                     rr1.at[c % 2, c // 4, d - 1], peer(d))

    def rs2(c, h):
        (m1, peer), _ = axes(c)
        return rcopy(p2s.at[c, (m1 + near[h]) % side], p2r.at[c, m1], s2.at[c, h], r2.at[c, h], peer(near[h]))

    def rs2x(c, h):
        (m1, peer), _ = axes(c)
        return rcopy(p2s.at[c, (m1 + 2) % side, part(h)], p2x.at[c, h], s2.at[c, 2 + h], r2.at[c, 2 + h], peer(near[h]))

    def rs2f(c, h):
        (m1, peer), _ = axes(c)
        a = (m1 + side - near[h]) % side
        return rcopy(p2x.at[c, h], p2r.at[c, a, part(h)], s2.at[c, 4 + h], r2.at[c, 4 + h], peer(near[h]))

    def rl2(c, d):
        (m1, peer), _ = axes(c)
        return rcopy(l2s.at[c % 2, both(c)], l2r.at[c % 2, m1, both(c)], sl2.at[c % 2, c // 4, d - 1],
                     rr2.at[c % 2, c // 4, d - 1], peer(d))

    def cload(b):
        return pltpu.make_async_copy(cache_ref.at[seq(b)], cbuf.at[b % NBUF], csem.at[b % NBUF])

    for b in range(min(NBUF, total)):
        cload(b).start()

    barrier = pltpu.get_barrier_semaphore()
    peers = [sib] + [at(y, (x + d) % side, core) for d in dists] + [at((y + d) % side, x, core) for d in dists]
    for dev in peers:
        pl.semaphore_signal(barrier, inc=1, device_id=dev, device_id_type=pl.DeviceIdType.MESH)
    pl.semaphore_wait(barrier, len(peers))

    def gather_far_rows(p):
        for ty in range(2):
            for h in range(2):
                ag1f(p, ty, h).wait_recv()

    for p in pieces:
        for ty in range(2):
            for h in range(2):
                ag1(p, ty, h).start()
    for p in pieces:
        for ty in range(2):
            (m1, _), _ = axes(ty)
            g1[ty, m1, bounds[p]:bounds[p + 1]] = q_ref[ty * each_type + bounds[p]:ty * each_type + bounds[p + 1]]
            for h in range(2):
                ag1(p, ty, h).wait_recv()
                ag1f(p, ty, h).start()
    gather_far_rows(0)

    def gather_first(c):
        _, (m2, _) = axes(c)
        if len(pieces) > 1:
            @pl.when(c == 2 * bounds[1] // nb)
            def _():
                gather_far_rows(1)

        def body(i, _):
            parts = [g1[c % 2, a, row(c) + i].astype(jnp.float32) for a in range(side)]
            qall[c, m2, i] = jnp.concatenate(parts, axis=0).astype(qall.dtype)
            return 0

        lax.fori_loop(0, nb, body, 0)
        for h in range(2):
            ag2(c, h).start()
        ag3(c, 0).start()

    def gather_second(c):
        for h in range(2):
            ag2(c, h).wait_recv()
            ag2f(c, h).start()
            ag3(c, near[h]).start()

    def gather_far(c):
        for h in range(2):
            ag2f(c, h).wait_recv()
        ag3(c, 2).start()

    def gather_third(c):
        for d in range(side):
            ag3(c, d).wait_recv()

    tpos = lax.broadcasted_iota(jnp.int32, (1, t), 1)
    pos = (tpos // page) * (page * n) + me * page + tpos % page

    def scores(b, ref):
        ref[...] = lax.dot_general(qall[b // nb, :, b % nb].reshape(2 * half, k), cbuf[b % NBUF],
                                   (((1,), (1,)), ((), ())), preferred_element_type=jnp.float32)

    def attend(c, i, ref):
        b = c * nb + i
        s = jnp.where(pos < lens_ref[seq(b)], ref[...], NEG)
        m = jnp.max(s, axis=1, keepdims=True)
        ms = jnp.where(m == NEG, 0.0, m)
        p = jnp.exp((s - ms) * SCALE)
        l = jnp.sum(p, axis=1, keepdims=True)
        acc = lax.dot_general(p.astype(jnp.bfloat16), cbuf[b % NBUF, :, :lorav], (((1,), (0,)), ((), ())),
                              preferred_element_type=jnp.float32)
        ls = jnp.where(l > 0.0, l, 1.0)
        o = acc * (1.0 / ls)
        lse = jnp.broadcast_to(jnp.where(l > 0.0, ms * SCALE + jnp.log(ls), NEG), (2 * half, LANES))
        own[c % NSLOT, i, :, :lorav] = o[:half]
        own[c % NSLOT, i, :, lorav:] = lse[:half]
        osend[c % NSLOT, i, :, :lorav] = o[half:]
        osend[c % NSLOT, i, :, lorav:] = lse[half:]

    diag = lax.broadcasted_iota(jnp.int32, (half, LANES), 0) == lax.broadcasted_iota(jnp.int32, (half, LANES), 1)

    def pair_one(c, i):
        la = own[c % NSLOT, i, :, lorav:]
        lb = orecv[c, i, :, lorav:]
        top = jnp.maximum(la, lb)
        ts = jnp.where(top == NEG, 0.0, top)
        wa = jnp.exp(la - ts)
        wb = jnp.exp(lb - ts)
        ws = wa + wb
        wss = jnp.where(ws > 0.0, ws, 1.0)
        inv = 1.0 / wss
        wa = wa * inv
        wb = wb * inv
        for j in range(lorav // LANES):
            cols = slice(j * LANES, (j + 1) * LANES)
            v = (wa * own[c % NSLOT, i, :, cols] + wb * orecv[c, i, :, cols]).astype(jnp.bfloat16)
            p1s[c, :, i, :, cols] = v.reshape(side, tile, LANES)
        lse = jnp.where(ws > 0.0, ts + jnp.log(wss), NEG)
        l1s[c % 2, c // 2, pl.ds(i, 1)] = jnp.sum(jnp.where(diag, lse, 0.0), axis=0, keepdims=True)

    def compute(c):
        @pl.when(c >= NSLOT)
        def _():
            od(c - NSLOT).wait_send()

        @pl.when(c == 0)
        def _():
            cload(0).wait()
            scores(0, sb0)

        def two(j, merged):
            b = c * nb + 2 * j
            cload(b + 1).wait()

            @pl.when(b + 2 < total)
            def _():
                cload(b + 2).wait()

            scores(b + 1, sb1)
            if merged:
                pair_one(jnp.maximum(c - LAG, 0), 2 * j)
                pair_one(jnp.maximum(c - LAG, 0), 2 * j + 1)
            attend(c, 2 * j, sb0)
            scores(jnp.minimum(b + 2, total - 1), sb0)
            attend(c, 2 * j + 1, sb1)
            for later in range(NBUF, NBUF + 2):
                @pl.when(b + later < total)
                def _():
                    cload(b + later).start()

            return 0

        @pl.when(c < LAG)
        def _():
            lax.fori_loop(0, nb // 2, lambda j, _: two(j, False), 0)

        @pl.when(c >= LAG)
        def _():
            od(jnp.maximum(c - LAG, 0)).wait_recv()
            lax.fori_loop(0, nb // 2, lambda j, _: two(j, True), 0)

        od(c).start()

    def pair(c):
        @pl.when(c >= nc - LAG)
        def _():
            od(c).wait_recv()

            def one(i, _):
                pair_one(c, i)
                return 0

            lax.fori_loop(0, nb, one, 0)

        for h in range(2):
            rs1x(c, h).start()

        @pl.when((c // 2) % 2 == 1)
        def _():
            for d in dists:
                rl1(c, d).start()

        for h in range(2):
            rs1(c, h).start()

    def pair_relay(c):
        for h in range(2):
            rs1x(c, h).wait_recv()
            rs1f(c, h).start()

    def weights(ls):
        top = functools.reduce(jnp.maximum, ls)
        ts = jnp.where(top == NEG, 0.0, top)
        w = [jnp.exp(v - ts) for v in ls]
        ws = functools.reduce(jnp.add, w)
        wss = jnp.where(ws > 0.0, ws, 1.0)
        inv = 1.0 / wss
        for j, v in enumerate(w):
            wrow[j] = v * inv
        return jnp.where(ws > 0.0, ts + jnp.log(wss), NEG)

    def combine(i, rows, first, srcs):
        sel = (lax.broadcasted_iota(jnp.int32, (rows, LANES), 0) + first
               == lax.broadcasted_iota(jnp.int32, (rows, LANES), 1))
        tot = None
        for j, src in enumerate(srcs):
            w = jnp.broadcast_to(wrow[j, pl.ds(i, 1)], (rows, LANES))
            w = jnp.sum(jnp.where(sel, w, 0.0), axis=1, keepdims=True)
            term = w * src[i].astype(jnp.float32)
            tot = term if tot is None else tot + term
        return tot

    def second(c):
        (m1, _), (m2, _) = axes(c)
        for h in range(2):
            rs1(c, h).wait_recv()
            rs1f(c, h).wait_recv()

        @pl.when((c // 2) % 2 == 0)
        def _():
            for d in dists:
                rl1(c, d).wait_recv()

        idx = [(m2 + d) % side for d in dists]
        l2s[c % 2, c // 2] = weights([l1s[c % 2, c // 2]] + [l1r[c % 2, a, c // 2] for a in idx])
        srcs = [p1s.at[c, m2]] + [p1r.at[c, a] for a in idx]

        def one(i, _):
            v = combine(i, tile, m2 * tile, srcs)
            for a in range(side):
                p2s[c, a, i] = v[a * hl:(a + 1) * hl]
            return 0

        lax.fori_loop(0, nb, one, 0)
        for h in range(2):
            rs2x(c, h).start()

        @pl.when((c // 2) % 2 == 1)
        def _():
            for d in dists:
                rl2(c, d).start()

        for h in range(2):
            rs2(c, h).start()

    def second_relay(c):
        for h in range(2):
            rs2x(c, h).wait_recv()
            rs2f(c, h).start()

    def final(c):
        (m1, _), (m2, _) = axes(c)
        for h in range(2):
            rs2(c, h).wait_recv()
            rs2f(c, h).wait_recv()

        @pl.when((c // 2) % 2 == 0)
        def _():
            for d in dists:
                rl2(c, d).wait_recv()

        idx = [(m1 + d) % side for d in dists]
        weights([l2s[c % 2, c // 2]] + [l2r[c % 2, a, c // 2] for a in idx])
        srcs = [p2s.at[c, m1]] + [p2r.at[c, a] for a in idx]

        def one(i, _):
            out_ref[seq(c * nb + i)] = combine(i, hl, m2 * tile + m1 * hl, srcs).astype(out_ref.dtype)
            return 0

        lax.fori_loop(0, nb, one, 0)

    def each(stage):
        def one(c, _):
            stage(c)
            return 0

        lax.fori_loop(0, nc, one, 0)

    stages = ((gather_third, 12), (compute, 13), (pair, 15), (gather_first, 0), (pair_relay, 18), (gather_second, 5),
              (gather_far, 9), (second, 23), (second_relay, 31), (final, 40))

    def step(i, _):
        for stage, delay in stages:
            @pl.when((i >= delay) & (i < delay + nc))
            def _():
                stage(jnp.maximum(i - delay, 0))

        return 0

    lax.fori_loop(0, nc + max(d for _, d in stages), step, 0)

    def drain(c):
        for h in range(2):
            for cp in (ag2, ag2f, rs1, rs1x, rs1f, rs2, rs2x, rs2f):
                cp(c, h).wait_send()

        @pl.when((c // 2) % 2 == 1)
        def _():
            for d in dists:
                rl1(c, d).wait_send()
                rl2(c, d).wait_send()

        for d in range(side):
            ag3(c, d).wait_send()

        @pl.when(c >= nc - NSLOT)
        def _():
            od(c).wait_send()

    each(drain)
    for p in pieces:
        for ty in range(2):
            for h in range(2):
                ag1(p, ty, h).wait_send()
                ag1f(p, ty, h).wait_send()


def solution(mesh):
    n = mesh.shape['dcp']
    side = math.isqrt(n // 2)

    def local(q, cache, lens):
        b, hl, k = q.shape
        t = cache.shape[1] * cache.shape[3]
        lorav = k - ROPE
        nb = min(4, max(1, b // 4))
        nc = b // nb
        tile = side * hl
        half = side * tile
        bf, f32 = jnp.bfloat16, jnp.float32
        dma = pltpu.SemaphoreType.DMA
        return pl.pallas_call(
            functools.partial(kernel, n, side, nc, nb, cache.shape[3]),
            out_shape=jax.ShapeDtypeStruct((b, hl, lorav), bf),
            in_specs=[pl.BlockSpec(memory_space=pltpu.VMEM), pl.BlockSpec(memory_space=pl.ANY),
                      pl.BlockSpec(memory_space=pltpu.SMEM)],
            out_specs=pl.BlockSpec(memory_space=pltpu.VMEM),
            scratch_shapes=[
                pltpu.VMEM((2, side, b // 2, hl, k), bf),
                pltpu.VMEM((nc, 2 * side, nb, tile, k), bf),
                pltpu.VMEM((NBUF, t, k), bf),
                pltpu.VMEM((NSLOT, nb, half, lorav + LANES), f32),
                pltpu.VMEM((NSLOT, nb, half, lorav + LANES), f32),
                pltpu.VMEM((nc, nb, half, lorav + LANES), f32),
                pltpu.VMEM((nc, side, nb, tile, lorav), bf),
                pltpu.VMEM((nc, 2, nb // 2, tile, lorav), bf),
                pltpu.VMEM((nc, side, nb, tile, lorav), bf),
                pltpu.VMEM((2, nc // 2, nb, LANES), f32),
                pltpu.VMEM((2, side, nc // 2, nb, LANES), f32),
                pltpu.VMEM((nc, side, nb, hl, lorav), f32),
                pltpu.VMEM((nc, 2, nb // 2, hl, lorav), f32),
                pltpu.VMEM((nc, side, nb, hl, lorav), f32),
                pltpu.VMEM((2, nc // 2, nb, LANES), f32),
                pltpu.VMEM((2, side, nc // 2, nb, LANES), f32),
                pltpu.VMEM((side, nb, LANES), f32),
                pltpu.VMEM((2 * half, t), f32), pltpu.VMEM((2 * half, t), f32),
                dma((NBUF,)),
                dma((2, 2, 4)), dma((2, 2, 4)), dma((nc, 4)), dma((nc, 4)),
                dma((nc, side)), dma((nc, side)),
                dma((nc,)), dma((nc,)),
                dma((nc, 6)), dma((nc, 6)), dma((2, nc // 4, side - 1)), dma((2, nc // 4, side - 1)),
                dma((nc, 6)), dma((nc, 6)), dma((2, nc // 4, side - 1)), dma((2, nc // 4, side - 1)),
            ],
            compiler_params=pltpu.CompilerParams(collective_id=0, has_side_effects=True,
                                                 vmem_limit_bytes=63 * 1024 * 1024),
        )(q, cache.reshape(b, t, k), lens)

    return jax.shard_map(local, mesh=mesh, in_specs=(P('dp', 'dcp', None), P('dp', None, 'dcp', None, None), P('dp')),
                         out_specs=P('dp', 'dcp', None), check_vma=False)
```

```python
import functools
import math

import jax
import jax.numpy as jnp
from jax import lax
from jax.experimental import pallas as pl
from jax.experimental.pallas import tpu as pltpu
from jax.sharding import PartitionSpec as P

ROPE = 64
QK_DIM = 192
SCALE = QK_DIM ** -0.5
NEG = float('-inf')
LANES = 128
NBUF = 6
NSLOT = 4
LAG = 2
LAST = 4


def kernel(n, side, nc, nb, page, q_ref, cache_ref, lens_ref, out_ref,
           g1, qall, cbuf, own, osend, orecv, p1s, p1x, p1r, l1s, l1r, p2s, p2x, p2r, l2s, l2r, wrow, sb0, sb1, ds, dr, dl, dlr, dsem,
           csem, a1s, a1r, a2s, a2r, a3s, a3r, ods, odr, s1, r1, sl1, rr1, s2, r2, sl2, rr2):
    hl = q_ref.shape[1]
    k = q_ref.shape[2]
    t = cbuf.shape[1]
    lorav = k - ROPE
    tile = side * hl
    half = side * tile
    total = nc * nb
    each_type = total // 2

    def row(c):
        return (c // 2) * nb

    def seq(b):
        c = b // nb
        return (c % 2) * each_type + row(c) + b % nb

    me = lax.axis_index('dcp')
    core = me % 2
    x = (me // 2) % side
    y = me // (2 * side)
    dists = tuple(range(1, side))

    def at(yy, xx, cc):
        return {'dcp': (yy * side + xx) * 2 + cc}

    sib = at(y, x, 1 - core)

    def axes(c):
        odd = c % 2
        return ((x + odd * (y - x), lambda d: at((y + odd * d) % side, (x + (1 - odd) * d) % side, core)),
                (y + odd * (x - y), lambda d: at((y + (1 - odd) * d) % side, (x + odd * d) % side, core)))

    def rcopy(src, dst, ss, rs, dev):
        return pltpu.make_async_remote_copy(src_ref=src, dst_ref=dst, send_sem=ss, recv_sem=rs, device_id=dev,
                                            device_id_type=pl.DeviceIdType.MESH)

    hb = nb // 2

    def part(h):
        return pl.ds(h * hb, hb)

    near = (1, side - 1)

    bounds = [0, min(2 * nb, each_type), each_type]
    pieces = [p for p in range(len(bounds) - 1) if bounds[p + 1] > bounds[p]]

    def ag1(p, ty, h):
        (m1, peer), _ = axes(ty)
        at_ = pl.ds(bounds[p], bounds[p + 1] - bounds[p])
        return rcopy(q_ref.at[pl.ds(ty * each_type + bounds[p], bounds[p + 1] - bounds[p])], g1.at[ty, m1, at_],
                     a1s.at[p, ty, h], a1r.at[p, ty, h], peer(near[h]))

    def ag1f(p, ty, h):
        (m1, peer), _ = axes(ty)
        a = (m1 + side - near[h]) % side
        size = (bounds[p + 1] - bounds[p]) // 2
        at_ = pl.ds(bounds[p] + h * size, size)
        return rcopy(g1.at[ty, a, at_], g1.at[ty, a, at_], a1s.at[p, ty, 2 + h], a1r.at[p, ty, 2 + h], peer(near[h]))

    def ag2(c, h):
        _, (m2, peer) = axes(c)
        return rcopy(qall.at[c, m2], qall.at[c, m2], a2s.at[c, h], a2r.at[c, h], peer(near[h]))

    def ag2f(c, h):
        _, (m2, peer) = axes(c)
        a = (m2 + side - near[h]) % side
        return rcopy(qall.at[c, a, part(h)], qall.at[c, a, part(h)], a2s.at[c, 2 + h], a2r.at[c, 2 + h], peer(near[h]))

    def ag3(c, d):
        _, (m2, _) = axes(c)
        a = (m2 + side - d) % side
        return rcopy(qall.at[c, a], qall.at[c, side + a], a3s.at[c, d], a3r.at[c, d], sib)

    def od(c):
        return rcopy(osend.at[c % NSLOT], orecv.at[c], ods.at[c], odr.at[c], sib)

    def rs1(c, h):
        _, (m2, peer) = axes(c)
        return rcopy(p1s.at[c, (m2 + near[h]) % side], p1r.at[c, m2], s1.at[c, h], r1.at[c, h], peer(near[h]))

    def rs1x(c, h):
        _, (m2, peer) = axes(c)
        return rcopy(p1s.at[c, (m2 + 2) % side, part(h)], p1x.at[c, h], s1.at[c, 2 + h], r1.at[c, 2 + h], peer(near[h]))

    def rs1f(c, h):
        _, (m2, peer) = axes(c)
        a = (m2 + side - near[h]) % side
        return rcopy(p1x.at[c, h], p1r.at[c, a, part(h)], s1.at[c, 4 + h], r1.at[c, 4 + h], peer(near[h]))

    def both(c):
        return pl.ds((c // 4) * 2, 2)

    def rl1(c, d):
        _, (m2, peer) = axes(c)
        return rcopy(l1s.at[c % 2, both(c)], l1r.at[c % 2, m2, both(c)], sl1.at[c % 2, c // 4, d - 1],
                     rr1.at[c % 2, c // 4, d - 1], peer(d))

    def rs2(c, h):
        (m1, peer), _ = axes(c)
        return rcopy(p2s.at[c, (m1 + near[h]) % side], p2r.at[c, m1], s2.at[c, h], r2.at[c, h], peer(near[h]))

    def rs2x(c, h):
        (m1, peer), _ = axes(c)
        return rcopy(p2s.at[c, (m1 + 2) % side, part(h)], p2x.at[c, h], s2.at[c, 2 + h], r2.at[c, 2 + h], peer(near[h]))

    def rs2f(c, h):
        (m1, peer), _ = axes(c)
        a = (m1 + side - near[h]) % side
        return rcopy(p2x.at[c, h], p2r.at[c, a, part(h)], s2.at[c, 4 + h], r2.at[c, 4 + h], peer(near[h]))

    def rl2(c, d):
        (m1, peer), _ = axes(c)
        return rcopy(l2s.at[c % 2, both(c)], l2r.at[c % 2, m1, both(c)], sl2.at[c % 2, c // 4, d - 1],
                     rr2.at[c % 2, c // 4, d - 1], peer(d))

    def cload(b):
        return pltpu.make_async_copy(cache_ref.at[seq(b)], cbuf.at[b % NBUF], csem.at[b % NBUF])

    for b in range(min(NBUF, total)):
        cload(b).start()

    barrier = pltpu.get_barrier_semaphore()
    peers = [sib] + [at((y + d // side) % side, (x + d % side) % side, core) for d in range(1, side * side)]
    for dev in peers:
        pl.semaphore_signal(barrier, inc=1, device_id=dev, device_id_type=pl.DeviceIdType.MESH)
    pl.semaphore_wait(barrier, len(peers))

    def gather_far_rows(p):
        for ty in range(2):
            for h in range(2):
                ag1f(p, ty, h).wait_recv()

    for p in pieces:
        for ty in range(2):
            for h in range(2):
                ag1(p, ty, h).start()
    for p in pieces:
        for ty in range(2):
            (m1, _), _ = axes(ty)
            g1[ty, m1, bounds[p]:bounds[p + 1]] = q_ref[ty * each_type + bounds[p]:ty * each_type + bounds[p + 1]]
            for h in range(2):
                ag1(p, ty, h).wait_recv()
                ag1f(p, ty, h).start()
    gather_far_rows(0)

    def gather_first(c):
        _, (m2, _) = axes(c)
        if len(pieces) > 1:
            @pl.when(c == 2 * bounds[1] // nb)
            def _():
                gather_far_rows(1)

        def body(i, _):
            parts = [g1[c % 2, a, row(c) + i].astype(jnp.float32) for a in range(side)]
            qall[c, m2, i] = jnp.concatenate(parts, axis=0).astype(qall.dtype)
            return 0

        lax.fori_loop(0, nb, body, 0)
        for h in range(2):
            ag2(c, h).start()
        ag3(c, 0).start()

    def gather_second(c):
        for h in range(2):
            ag2(c, h).wait_recv()
            ag2f(c, h).start()
            ag3(c, near[h]).start()

    def gather_far(c):
        for h in range(2):
            ag2f(c, h).wait_recv()
        ag3(c, 2).start()

    def gather_third(c):
        for d in range(side):
            ag3(c, d).wait_recv()

    tpos = lax.broadcasted_iota(jnp.int32, (1, t), 1)
    pos = (tpos // page) * (page * n) + me * page + tpos % page

    def scores(b, ref):
        ref[...] = lax.dot_general(qall[b // nb, :, b % nb].reshape(2 * half, k), cbuf[b % NBUF],
                                   (((1,), (1,)), ((), ())), preferred_element_type=jnp.float32)

    def attend(c, i, ref):
        b = c * nb + i
        s = jnp.where(pos < lens_ref[seq(b)], ref[...], NEG)
        m = jnp.max(s, axis=1, keepdims=True)
        ms = jnp.where(m == NEG, 0.0, m)
        p = jnp.exp((s - ms) * SCALE)
        l = jnp.sum(p, axis=1, keepdims=True)
        acc = lax.dot_general(p.astype(jnp.bfloat16), cbuf[b % NBUF, :, :lorav], (((1,), (0,)), ((), ())),
                              preferred_element_type=jnp.float32)
        ls = jnp.where(l > 0.0, l, 1.0)
        o = acc * (1.0 / ls)
        lse = jnp.broadcast_to(jnp.where(l > 0.0, ms * SCALE + jnp.log(ls), NEG), (2 * half, LANES))
        own[c % NSLOT, i, :, :lorav] = o[:half]
        own[c % NSLOT, i, :, lorav:] = lse[:half]
        osend[c % NSLOT, i, :, :lorav] = o[half:]
        osend[c % NSLOT, i, :, lorav:] = lse[half:]

    diag = lax.broadcasted_iota(jnp.int32, (half, LANES), 0) == lax.broadcasted_iota(jnp.int32, (half, LANES), 1)

    def pair_one(c, i, direct=False):
        la = own[c % NSLOT, i, :, lorav:]
        lb = orecv[c, i, :, lorav:]
        top = jnp.maximum(la, lb)
        ts = jnp.where(top == NEG, 0.0, top)
        wa = jnp.exp(la - ts)
        wb = jnp.exp(lb - ts)
        ws = wa + wb
        wss = jnp.where(ws > 0.0, ws, 1.0)
        inv = 1.0 / wss
        wa = wa * inv
        wb = wb * inv
        for j in range(lorav // LANES):
            cols = slice(j * LANES, (j + 1) * LANES)
            v = wa * own[c % NSLOT, i, :, cols] + wb * orecv[c, i, :, cols]
            if direct:
                for a in range(side * side):
                    ds[c - (nc - LAST), a, i, :, cols] = v[a * hl:(a + 1) * hl].astype(jnp.bfloat16)
            else:
                p1s[c, :, i, :, cols] = v.astype(jnp.bfloat16).reshape(side, tile, LANES)
        lse = jnp.where(ws > 0.0, ts + jnp.log(wss), NEG)
        lrow = jnp.sum(jnp.where(diag, lse, 0.0), axis=0, keepdims=True)
        if direct:
            dl[c - (nc - LAST), pl.ds(i, 1)] = lrow
        else:
            l1s[c % 2, c // 2, pl.ds(i, 1)] = lrow

    def compute(c):
        @pl.when(c >= NSLOT)
        def _():
            od(c - NSLOT).wait_send()

        @pl.when(c == 0)
        def _():
            cload(0).wait()
            scores(0, sb0)

        def two(j, merged):
            b = c * nb + 2 * j
            cload(b + 1).wait()

            @pl.when(b + 2 < total)
            def _():
                cload(b + 2).wait()

            scores(b + 1, sb1)
            if merged:
                pair_one(jnp.maximum(c - LAG, 0), 2 * j)
                pair_one(jnp.maximum(c - LAG, 0), 2 * j + 1)
            attend(c, 2 * j, sb0)
            scores(jnp.minimum(b + 2, total - 1), sb0)
            attend(c, 2 * j + 1, sb1)
            for later in range(NBUF, NBUF + 2):
                @pl.when(b + later < total)
                def _():
                    cload(b + later).start()

            return 0

        merged = (c >= LAG) & (c < nc - LAST + LAG)

        @pl.when(jnp.logical_not(merged))
        def _():
            lax.fori_loop(0, nb // 2, lambda j, _: two(j, False), 0)

        @pl.when(merged)
        def _():
            od(jnp.maximum(c - LAG, 0)).wait_recv()
            lax.fori_loop(0, nb // 2, lambda j, _: two(j, True), 0)

        od(c).start()

    def far_peer(c, k):
        yy, xx = (y + k // side) % side, (x + k % side) % side
        return c % 2 * (xx * side + yy) + (1 - c % 2) * (yy * side + xx), at(yy, xx, core)

    def direct(c, k):
        u = c - (nc - LAST)
        slot, dev = far_peer(c, k)
        return (rcopy(ds.at[u, slot], dr.at[u, k - 1], dsem.at[0, u], dsem.at[1, u], dev),
                rcopy(dl.at[u], dlr.at[u, k - 1], dsem.at[2, u], dsem.at[3, u], dev))

    def direct_all(u):
        many = pl.ds(0, side * side - 1)
        return (rcopy(ds.at[u, many], dr.at[u, many], dsem.at[0, u], dsem.at[1, u], sib),
                rcopy(dlr.at[u, many], dlr.at[u, many], dsem.at[2, u], dsem.at[3, u], sib))

    def pair(c):
        @pl.when(c < nc - LAST)
        def _():
            pair_send(c)

        @pl.when(c >= nc - LAST)
        def _():
            tail = jnp.maximum(c, nc - LAST)
            od(tail).wait_recv()

            def one(i, _):
                pair_one(tail, i, direct=True)
                return 0

            lax.fori_loop(0, nb, one, 0)

            def send(k, _):
                for cp in direct(tail, k):
                    cp.start()
                return 0

            lax.fori_loop(1, side * side, send, 0)

    def pair_send(c):
        for h in range(2):
            rs1x(c, h).start()

        @pl.when((c // 2) % 2 == 1)
        def _():
            for d in dists:
                rl1(c, d).start()

        for h in range(2):
            rs1(c, h).start()

    def pair_relay(c):
        for h in range(2):
            rs1x(c, h).wait_recv()
            rs1f(c, h).start()

    def weights(ls):
        top = functools.reduce(jnp.maximum, ls)
        ts = jnp.where(top == NEG, 0.0, top)
        w = [jnp.exp(v - ts) for v in ls]
        ws = functools.reduce(jnp.add, w)
        wss = jnp.where(ws > 0.0, ws, 1.0)
        inv = 1.0 / wss
        for j, v in enumerate(w):
            wrow[j] = v * inv
        return jnp.where(ws > 0.0, ts + jnp.log(wss), NEG)

    def combine(i, rows, first, srcs):
        sel = (lax.broadcasted_iota(jnp.int32, (rows, LANES), 0) + first
               == lax.broadcasted_iota(jnp.int32, (rows, LANES), 1))
        tot = None
        for j, src in enumerate(srcs):
            w = jnp.broadcast_to(wrow[j, pl.ds(i, 1)], (rows, LANES))
            w = jnp.sum(jnp.where(sel, w, 0.0), axis=1, keepdims=True)
            term = w * src[i].astype(jnp.float32)
            tot = term if tot is None else tot + term
        return tot

    def second(c):
        (m1, _), (m2, _) = axes(c)
        for h in range(2):
            rs1(c, h).wait_recv()
            rs1f(c, h).wait_recv()

        @pl.when((c // 2) % 2 == 0)
        def _():
            for d in dists:
                rl1(c, d).wait_recv()

        idx = [(m2 + d) % side for d in dists]
        l2s[c % 2, c // 2] = weights([l1s[c % 2, c // 2]] + [l1r[c % 2, a, c // 2] for a in idx])
        srcs = [p1s.at[c, m2]] + [p1r.at[c, a] for a in idx]

        def one(i, _):
            v = combine(i, tile, m2 * tile, srcs)
            for a in range(side):
                p2s[c, a, i] = v[a * hl:(a + 1) * hl]
            return 0

        lax.fori_loop(0, nb, one, 0)
        for h in range(2):
            rs2x(c, h).start()

        @pl.when((c // 2) % 2 == 1)
        def _():
            for d in dists:
                rl2(c, d).start()

        for h in range(2):
            rs2(c, h).start()

    def second_relay(c):
        for h in range(2):
            rs2x(c, h).wait_recv()
            rs2f(c, h).start()

    def final(c):
        (m1, _), (m2, _) = axes(c)
        for h in range(2):
            rs2(c, h).wait_recv()
            rs2f(c, h).wait_recv()

        @pl.when((c // 2) % 2 == 0)
        def _():
            for d in dists:
                rl2(c, d).wait_recv()

        idx = [(m1 + d) % side for d in dists]
        weights([l2s[c % 2, c // 2]] + [l2r[c % 2, a, c // 2] for a in idx])
        srcs = [p2s.at[c, m1]] + [p2r.at[c, a] for a in idx]

        def one(i, _):
            out_ref[seq(c * nb + i)] = combine(i, hl, m2 * tile + m1 * hl, srcs).astype(out_ref.dtype)
            return 0

        lax.fori_loop(0, nb, one, 0)

    def final_direct(c):
        (m1, _), (m2, _) = axes(c)
        u = c - (nc - LAST)
        for cp in direct_all(u):
            cp.wait_recv()
        count = side * side - 1
        weights([dl[u]] + [dlr[u, a] for a in range(count)])
        srcs = [ds.at[u, m2 * side + m1]] + [dr.at[u, a] for a in range(count)]

        def one(i, _):
            out_ref[seq(c * nb + i)] = combine(i, hl, m2 * tile + m1 * hl, srcs).astype(out_ref.dtype)
            return 0

        lax.fori_loop(0, nb, one, 0)

    def each(stage):
        def one(c, _):
            stage(c)
            return 0

        lax.fori_loop(0, nc, one, 0)

    mid = nc - LAST
    stages = ((gather_third, 12, nc), (compute, 13, nc), (pair, 15, nc), (gather_first, 0, nc), (pair_relay, 18, mid),
              (gather_second, 5, nc), (gather_far, 9, nc), (second, 23, mid), (second_relay, 29, mid), (final, 36, mid))

    def step(i, _):
        for stage, delay, count in stages:
            @pl.when((i >= delay) & (i < delay + count))
            def _():
                stage(jnp.maximum(i - delay, 0))

        return 0

    lax.fori_loop(0, max(delay + count for _, delay, count in stages), step, 0)

    def last(u, _):
        final_direct(u + mid)
        return 0

    lax.fori_loop(0, LAST, last, 0)

    def drain(c):
        for h in range(2):
            ag2(c, h).wait_send()
            ag2f(c, h).wait_send()
        for d in range(side):
            ag3(c, d).wait_send()

        @pl.when(c < mid)
        def _():
            for h in range(2):
                for cp in (rs1, rs1x, rs1f, rs2, rs2x, rs2f):
                    cp(c, h).wait_send()

        @pl.when((c < mid) & ((c // 2) % 2 == 1))
        def _():
            for d in dists:
                rl1(c, d).wait_send()
                rl2(c, d).wait_send()

        @pl.when(c >= nc - NSLOT)
        def _():
            od(c).wait_send()

    each(drain)
    for u in range(LAST):
        for cp in direct_all(u):
            cp.wait_send()
    for p in pieces:
        for ty in range(2):
            for h in range(2):
                ag1(p, ty, h).wait_send()
                ag1f(p, ty, h).wait_send()


def solution(mesh):
    n = mesh.shape['dcp']
    side = math.isqrt(n // 2)

    def local(q, cache, lens):
        b, hl, k = q.shape
        t = cache.shape[1] * cache.shape[3]
        lorav = k - ROPE
        nb = min(4, max(1, b // 4))
        nc = b // nb
        tile = side * hl
        half = side * tile
        bf, f32 = jnp.bfloat16, jnp.float32
        dma = pltpu.SemaphoreType.DMA
        return pl.pallas_call(
            functools.partial(kernel, n, side, nc, nb, cache.shape[3]),
            out_shape=jax.ShapeDtypeStruct((b, hl, lorav), bf),
            in_specs=[pl.BlockSpec(memory_space=pltpu.VMEM), pl.BlockSpec(memory_space=pl.ANY),
                      pl.BlockSpec(memory_space=pltpu.SMEM)],
            out_specs=pl.BlockSpec(memory_space=pltpu.VMEM),
            scratch_shapes=[
                pltpu.VMEM((2, side, b // 2, hl, k), bf),
                pltpu.VMEM((nc, 2 * side, nb, tile, k), bf),
                pltpu.VMEM((NBUF, t, k), bf),
                pltpu.VMEM((NSLOT, nb, half, lorav + LANES), f32),
                pltpu.VMEM((NSLOT, nb, half, lorav + LANES), f32),
                pltpu.VMEM((nc, nb, half, lorav + LANES), f32),
                pltpu.VMEM((nc, side, nb, tile, lorav), bf),
                pltpu.VMEM((nc, 2, nb // 2, tile, lorav), bf),
                pltpu.VMEM((nc, side, nb, tile, lorav), bf),
                pltpu.VMEM((2, nc // 2, nb, LANES), f32),
                pltpu.VMEM((2, side, nc // 2, nb, LANES), f32),
                pltpu.VMEM((nc, side, nb, hl, lorav), f32),
                pltpu.VMEM((nc, 2, nb // 2, hl, lorav), f32),
                pltpu.VMEM((nc, side, nb, hl, lorav), f32),
                pltpu.VMEM((2, nc // 2, nb, LANES), f32),
                pltpu.VMEM((2, side, nc // 2, nb, LANES), f32),
                pltpu.VMEM((side * side, nb, LANES), f32),
                pltpu.VMEM((2 * half, t), f32), pltpu.VMEM((2 * half, t), f32),
                pltpu.VMEM((LAST, side * side, nb, hl, lorav), bf),
                pltpu.VMEM((LAST, side * side - 1, nb, hl, lorav), bf),
                pltpu.VMEM((LAST, nb, LANES), f32),
                pltpu.VMEM((LAST, side * side - 1, nb, LANES), f32),
                dma((4, LAST)),
                dma((NBUF,)),
                dma((2, 2, 4)), dma((2, 2, 4)), dma((nc, 4)), dma((nc, 4)),
                dma((nc, side)), dma((nc, side)),
                dma((nc,)), dma((nc,)),
                dma((nc, 6)), dma((nc, 6)), dma((2, nc // 4, side - 1)), dma((2, nc // 4, side - 1)),
                dma((nc, 6)), dma((nc, 6)), dma((2, nc // 4, side - 1)), dma((2, nc // 4, side - 1)),
            ],
            compiler_params=pltpu.CompilerParams(collective_id=0, has_side_effects=True,
                                                 vmem_limit_bytes=63 * 1024 * 1024),
        )(q, cache.reshape(b, t, k), lens)

    return jax.shard_map(local, mesh=mesh, in_specs=(P('dp', 'dcp', None), P('dp', None, 'dcp', None, None), P('dp')),
                         out_specs=P('dp', 'dcp', None), check_vma=False)
```

```python
import functools
import math

import jax
import jax.numpy as jnp
from jax import lax
from jax.experimental import pallas as pl
from jax.experimental.pallas import tpu as pltpu
from jax.sharding import PartitionSpec as P

ROPE = 64
QK_DIM = 192
SCALE = QK_DIM ** -0.5
NEG = float('-inf')
LANES = 128
NBUF = 8
NSLOT = 4
LAG = 2


def mod(a, b):
    return a % b if isinstance(a, int) else lax.rem(a, b)


def div(a, b):
    return a // b if isinstance(a, int) else lax.div(a, b)


def kernel(n, side, nc, nb, page, q_ref, cache_ref, lens_ref, out_ref,
           g1, qall, cbuf, own, osend, orecv, p1s, p1x, p1r, l1s, l1r, p2s, p2x, p2r, l2s, l2r, wrow, sb0, sb1,
           csem, a1s, a1r, a2s, a2r, a3s, a3r, ods, odr, s1, r1, sl1, rr1, s2, r2, sl2, rr2):
    hl = q_ref.shape[1]
    k = q_ref.shape[2]
    t = cbuf.shape[1]
    lorav = k - ROPE
    tile = side * hl
    half = side * tile
    total = nc * nb
    each_type = total // 2

    def row(c):
        return (div(c, 2)) * nb

    def seq(b):
        c = div(b, nb)
        return (mod(c, 2)) * each_type + row(c) + mod(b, nb)

    me = lax.axis_index('dcp')
    core = me % 2
    x = (me // 2) % side
    y = me // (2 * side)
    dists = tuple(range(1, side))

    def at(yy, xx, cc):
        return {'dcp': (yy * side + xx) * 2 + cc}

    sib = at(y, x, 1 - core)

    xs = [(x + d) % side for d in range(side)]
    ys = [(y + d) % side for d in range(side)]
    xid = [(y * side + v) * 2 + core for v in xs]
    yid = [(v * side + x) * 2 + core for v in ys]

    def pos_at(c, axis, d):
        odd = mod(c, 2) if axis == 0 else 1 - mod(c, 2)
        return xs[d] + odd * (ys[d] - xs[d])

    def axes(c):
        def along(axis):
            odd = mod(c, 2) if axis == 0 else 1 - mod(c, 2)
            return pos_at(c, axis, 0), lambda d: {'dcp': xid[d] + odd * (yid[d] - xid[d])}

        return along(0), along(1)

    def rcopy(src, dst, ss, rs, dev):
        return pltpu.make_async_remote_copy(src_ref=src, dst_ref=dst, send_sem=ss, recv_sem=rs, device_id=dev,
                                            device_id_type=pl.DeviceIdType.MESH)

    hb = nb // 2

    def part(h):
        return pl.ds(h * hb, hb)

    near = (1, side - 1)

    bounds = [0, min(2 * nb, each_type), each_type]
    pieces = [p for p in range(len(bounds) - 1) if bounds[p + 1] > bounds[p]]

    def ag1(p, ty, h):
        (m1, peer), _ = axes(ty)
        at_ = pl.ds(bounds[p], bounds[p + 1] - bounds[p])
        return rcopy(q_ref.at[pl.ds(ty * each_type + bounds[p], bounds[p + 1] - bounds[p])], g1.at[ty, m1, at_],
                     a1s.at[p, ty, h], a1r.at[p, ty, h], peer(near[h]))

    def ag1f(p, ty, h):
        (m1, peer), _ = axes(ty)
        a = (m1 + side - near[h]) % side
        size = (bounds[p + 1] - bounds[p]) // 2
        at_ = pl.ds(bounds[p] + h * size, size)
        return rcopy(g1.at[ty, a, at_], g1.at[ty, a, at_], a1s.at[p, ty, 2 + h], a1r.at[p, ty, 2 + h], peer(near[h]))

    def ag2(c, h):
        _, (m2, peer) = axes(c)
        return rcopy(qall.at[c, m2], qall.at[c, m2], a2s.at[c, h], a2r.at[c, h], peer(near[h]))

    def ag2f(c, h):
        _, (_, peer) = axes(c)
        a = pos_at(c, 1, near[1 - h])
        return rcopy(qall.at[c, a, part(h)], qall.at[c, a, part(h)], a2s.at[c, 2 + h], a2r.at[c, 2 + h], peer(near[h]))

    def ag3(c, d):
        a = pos_at(c, 1, (side - d) % side)
        return rcopy(qall.at[c, a], qall.at[c, side + a], a3s.at[c, d], a3r.at[c, d], sib)

    def od(c):
        return rcopy(osend.at[mod(c, NSLOT)], orecv.at[c], ods.at[c], odr.at[c], sib)

    def rs1(c, h):
        _, (m2, peer) = axes(c)
        return rcopy(p1s.at[c, pos_at(c, 1, near[h])], p1r.at[c, m2], s1.at[c, h], r1.at[c, h], peer(near[h]))

    def rs1x(c, h):
        _, (m2, peer) = axes(c)
        return rcopy(p1s.at[c, pos_at(c, 1, 2), part(h)], p1x.at[c, h], s1.at[c, 2 + h], r1.at[c, 2 + h], peer(near[h]))

    def rs1f(c, h):
        _, (m2, peer) = axes(c)
        a = pos_at(c, 1, near[1 - h])
        return rcopy(p1x.at[c, h], p1r.at[c, a, part(h)], s1.at[c, 4 + h], r1.at[c, 4 + h], peer(near[h]))

    def both(c):
        return pl.ds((div(c, 4)) * 2, 2)

    def rl1(c, d):
        _, (m2, peer) = axes(c)
        return rcopy(l1s.at[mod(c, 2), both(c)], l1r.at[mod(c, 2), m2, both(c)], sl1.at[mod(c, 2), div(c, 4), d - 1],
                     rr1.at[mod(c, 2), div(c, 4), d - 1], peer(d))

    def rs2(c, h):
        (m1, peer), _ = axes(c)
        return rcopy(p2s.at[c, pos_at(c, 0, near[h])], p2r.at[c, m1], s2.at[c, h], r2.at[c, h], peer(near[h]))

    def rs2x(c, h):
        (m1, peer), _ = axes(c)
        return rcopy(p2s.at[c, pos_at(c, 0, 2), part(h)], p2x.at[c, h], s2.at[c, 2 + h], r2.at[c, 2 + h], peer(near[h]))

    def rs2f(c, h):
        (m1, peer), _ = axes(c)
        a = pos_at(c, 0, near[1 - h])
        return rcopy(p2x.at[c, h], p2r.at[c, a, part(h)], s2.at[c, 4 + h], r2.at[c, 4 + h], peer(near[h]))

    def rl2(c, d):
        (m1, peer), _ = axes(c)
        return rcopy(l2s.at[mod(c, 2), both(c)], l2r.at[mod(c, 2), m1, both(c)], sl2.at[mod(c, 2), div(c, 4), d - 1],
                     rr2.at[mod(c, 2), div(c, 4), d - 1], peer(d))

    def cload(b):
        return pltpu.make_async_copy(cache_ref.at[seq(b)], cbuf.at[mod(b, NBUF)], csem.at[mod(b, NBUF)])

    for b in range(min(NBUF, total)):
        cload(b).start()

    barrier = pltpu.get_barrier_semaphore()
    peers = [sib] + [at(y, (x + d) % side, core) for d in dists] + [at((y + d) % side, x, core) for d in dists]
    for dev in peers:
        pl.semaphore_signal(barrier, inc=1, device_id=dev, device_id_type=pl.DeviceIdType.MESH)
    pl.semaphore_wait(barrier, len(peers))

    def gather_far_rows(p):
        for ty in range(2):
            for h in range(2):
                ag1f(p, ty, h).wait_recv()

    for p in pieces:
        for ty in range(2):
            for h in range(2):
                ag1(p, ty, h).start()
    for p in pieces:
        for ty in range(2):
            (m1, _), _ = axes(ty)
            g1[ty, m1, bounds[p]:bounds[p + 1]] = q_ref[ty * each_type + bounds[p]:ty * each_type + bounds[p + 1]]
            for h in range(2):
                ag1(p, ty, h).wait_recv()
                ag1f(p, ty, h).start()
    gather_far_rows(0)

    def gather_first(c):
        _, (m2, _) = axes(c)
        if len(pieces) > 1:
            @pl.when(c == 2 * bounds[1] // nb)
            def _():
                gather_far_rows(1)

        def body(i, _):
            parts = [g1[mod(c, 2), a, row(c) + i].astype(jnp.float32) for a in range(side)]
            qall[c, m2, i] = jnp.concatenate(parts, axis=0).astype(qall.dtype)
            return 0

        lax.fori_loop(0, nb, body, 0)
        for h in range(2):
            ag2(c, h).start()
        ag3(c, 0).start()

    def gather_second(c):
        for h in range(2):
            ag2(c, h).wait_recv()
            ag2f(c, h).start()
            ag3(c, near[h]).start()

    def gather_far(c):
        for h in range(2):
            ag2f(c, h).wait_recv()
        ag3(c, 2).start()

    def gather_third(c):
        for d in range(side):
            ag3(c, d).wait_recv()

    tpos = lax.broadcasted_iota(jnp.int32, (1, t), 1)
    pos = (tpos // page) * (page * n) + me * page + tpos % page

    def scores(b, ref):
        ref[...] = lax.dot_general(qall[div(b, nb), :, mod(b, nb)].reshape(2 * half, k), cbuf[mod(b, NBUF)],
                                   (((1,), (1,)), ((), ())), preferred_element_type=jnp.float32)

    def attend(c, i, ref):
        b = c * nb + i
        s = jnp.where(pos < lens_ref[seq(b)], ref[...], NEG)
        m = jnp.max(s, axis=1, keepdims=True)
        ms = jnp.where(m == NEG, 0.0, m)
        p = jnp.exp((s - ms) * SCALE)
        l = jnp.sum(p, axis=1, keepdims=True)
        acc = lax.dot_general(p.astype(jnp.bfloat16), cbuf[mod(b, NBUF), :, :lorav], (((1,), (0,)), ((), ())),
                              preferred_element_type=jnp.float32)
        ls = jnp.where(l > 0.0, l, 1.0)
        o = acc * (1.0 / ls)
        lse = jnp.broadcast_to(jnp.where(l > 0.0, ms * SCALE + jnp.log(ls), NEG), (2 * half, LANES))
        own[mod(c, NSLOT), i, :, :lorav] = o[:half]
        own[mod(c, NSLOT), i, :, lorav:] = lse[:half]
        osend[mod(c, NSLOT), i, :, :lorav] = o[half:]
        osend[mod(c, NSLOT), i, :, lorav:] = lse[half:]

    diag = lax.broadcasted_iota(jnp.int32, (half, LANES), 0) == lax.broadcasted_iota(jnp.int32, (half, LANES), 1)

    def pair_one(c, i):
        la = own[mod(c, NSLOT), i, :, lorav:]
        lb = orecv[c, i, :, lorav:]
        top = jnp.maximum(la, lb)
        ts = jnp.where(top == NEG, 0.0, top)
        wa = jnp.exp(la - ts)
        wb = jnp.exp(lb - ts)
        ws = wa + wb
        wss = jnp.where(ws > 0.0, ws, 1.0)
        inv = 1.0 / wss
        wa = wa * inv
        wb = wb * inv
        for j in range(lorav // LANES):
            cols = slice(j * LANES, (j + 1) * LANES)
            v = (wa * own[mod(c, NSLOT), i, :, cols] + wb * orecv[c, i, :, cols]).astype(jnp.bfloat16)
            p1s[c, :, i, :, cols] = v.reshape(side, tile, LANES)
        lse = jnp.where(ws > 0.0, ts + jnp.log(wss), NEG)
        l1s[mod(c, 2), div(c, 2), pl.ds(i, 1)] = jnp.sum(jnp.where(diag, lse, 0.0), axis=0, keepdims=True)

    def compute(c):
        @pl.when(c >= NSLOT)
        def _():
            od(jnp.maximum(c - NSLOT, 0)).wait_send()

        @pl.when(c == 0)
        def _():
            cload(0).wait()
            scores(0, sb0)

        def two(j, merged):
            b = c * nb + 2 * j
            cload(b + 1).wait()

            @pl.when(b + 2 < total)
            def _():
                cload(b + 2).wait()

            scores(b + 1, sb1)
            if merged:
                pair_one(jnp.maximum(c - LAG, 0), 2 * j)
                pair_one(jnp.maximum(c - LAG, 0), 2 * j + 1)
            attend(c, 2 * j, sb0)
            scores(jnp.minimum(b + 2, total - 1), sb0)
            attend(c, 2 * j + 1, sb1)
            for later in range(NBUF, NBUF + 2):
                @pl.when(b + later < total)
                def _():
                    cload(b + later).start()

            return 0

        @pl.when(c < LAG)
        def _():
            lax.fori_loop(0, nb // 2, lambda j, _: two(j, False), 0)

        @pl.when(c >= LAG)
        def _():
            od(jnp.maximum(c - LAG, 0)).wait_recv()
            lax.fori_loop(0, nb // 2, lambda j, _: two(j, True), 0)

        od(c).start()

    def pair(c):
        @pl.when(c >= nc - LAG)
        def _():
            od(c).wait_recv()

            def one(i, _):
                pair_one(c, i)
                return 0

            lax.fori_loop(0, nb, one, 0)

        for h in range(2):
            rs1x(c, h).start()

        @pl.when(mod(div(c, 2), 2) == 1)
        def _():
            for d in dists:
                rl1(c, d).start()

        for h in range(2):
            rs1(c, h).start()

    def pair_relay(c):
        for h in range(2):
            rs1x(c, h).wait_recv()
            rs1f(c, h).start()

    def weights(ls):
        top = functools.reduce(jnp.maximum, ls)
        ts = jnp.where(top == NEG, 0.0, top)
        w = [jnp.exp(v - ts) for v in ls]
        ws = functools.reduce(jnp.add, w)
        wss = jnp.where(ws > 0.0, ws, 1.0)
        inv = 1.0 / wss
        for j, v in enumerate(w):
            wrow[j] = v * inv
        return jnp.where(ws > 0.0, ts + jnp.log(wss), NEG)

    def combine(i, rows, first, srcs):
        sel = (lax.broadcasted_iota(jnp.int32, (rows, LANES), 0) + first
               == lax.broadcasted_iota(jnp.int32, (rows, LANES), 1))
        tot = None
        for j, src in enumerate(srcs):
            w = jnp.broadcast_to(wrow[j, pl.ds(i, 1)], (rows, LANES))
            w = jnp.sum(jnp.where(sel, w, 0.0), axis=1, keepdims=True)
            term = w * src[i].astype(jnp.float32)
            tot = term if tot is None else tot + term
        return tot

    def second(c):
        (m1, _), (m2, _) = axes(c)
        for h in range(2):
            rs1(c, h).wait_recv()
            rs1f(c, h).wait_recv()

        @pl.when(mod(div(c, 2), 2) == 0)
        def _():
            for d in dists:
                rl1(c, d).wait_recv()

        idx = [pos_at(c, 1, d) for d in dists]
        l2s[mod(c, 2), div(c, 2)] = weights([l1s[mod(c, 2), div(c, 2)]] + [l1r[mod(c, 2), a, div(c, 2)] for a in idx])
        srcs = [p1s.at[c, m2]] + [p1r.at[c, a] for a in idx]

        def one(i, _):
            v = combine(i, tile, m2 * tile, srcs)
            for a in range(side):
                p2s[c, a, i] = v[a * hl:(a + 1) * hl]
            return 0

        lax.fori_loop(0, nb, one, 0)
        for h in range(2):
            rs2x(c, h).start()

        @pl.when(mod(div(c, 2), 2) == 1)
        def _():
            for d in dists:
                rl2(c, d).start()

        for h in range(2):
            rs2(c, h).start()

    def second_relay(c):
        for h in range(2):
            rs2x(c, h).wait_recv()
            rs2f(c, h).start()

    def final(c):
        (m1, _), (m2, _) = axes(c)
        for h in range(2):
            rs2(c, h).wait_recv()
            rs2f(c, h).wait_recv()

        @pl.when(mod(div(c, 2), 2) == 0)
        def _():
            for d in dists:
                rl2(c, d).wait_recv()

        idx = [pos_at(c, 0, d) for d in dists]
        weights([l2s[mod(c, 2), div(c, 2)]] + [l2r[mod(c, 2), a, div(c, 2)] for a in idx])
        srcs = [p2s.at[c, m1]] + [p2r.at[c, a] for a in idx]

        def one(i, _):
            out_ref[seq(c * nb + i)] = combine(i, hl, m2 * tile + m1 * hl, srcs).astype(out_ref.dtype)
            return 0

        lax.fori_loop(0, nb, one, 0)

    def each(stage):
        def one(c, _):
            stage(c)
            return 0

        lax.fori_loop(0, nc, one, 0)

    stages = ((gather_third, 12), (compute, 13), (pair, 15), (gather_first, 0), (pair_relay, 18), (gather_second, 5),
              (gather_far, 9), (second, 23), (second_relay, 31), (final, 40))

    def step(i, _):
        for stage, delay in stages:
            @pl.when((i >= delay) & (i < delay + nc))
            def _():
                stage(jnp.maximum(i - delay, 0))

        return 0

    lax.fori_loop(0, nc + max(d for _, d in stages), step, 0)

    def drain(c):
        for h in range(2):
            for cp in (ag2, ag2f, rs1, rs1x, rs1f, rs2, rs2x, rs2f):
                cp(c, h).wait_send()

        @pl.when(mod(div(c, 2), 2) == 1)
        def _():
            for d in dists:
                rl1(c, d).wait_send()
                rl2(c, d).wait_send()

        for d in range(side):
            ag3(c, d).wait_send()

        @pl.when(c >= nc - NSLOT)
        def _():
            od(c).wait_send()

    each(drain)
    for p in pieces:
        for ty in range(2):
            for h in range(2):
                ag1(p, ty, h).wait_send()
                ag1f(p, ty, h).wait_send()


def solution(mesh):
    n = mesh.shape['dcp']
    side = math.isqrt(n // 2)

    def local(q, cache, lens):
        b, hl, k = q.shape
        t = cache.shape[1] * cache.shape[3]
        lorav = k - ROPE
        nb = min(4, max(1, b // 4))
        nc = div(b, nb)
        tile = side * hl
        half = side * tile
        bf, f32 = jnp.bfloat16, jnp.float32
        dma = pltpu.SemaphoreType.DMA
        return pl.pallas_call(
            functools.partial(kernel, n, side, nc, nb, cache.shape[3]),
            out_shape=jax.ShapeDtypeStruct((b, hl, lorav), bf),
            in_specs=[pl.BlockSpec(memory_space=pltpu.VMEM), pl.BlockSpec(memory_space=pl.ANY),
                      pl.BlockSpec(memory_space=pltpu.SMEM)],
            out_specs=pl.BlockSpec(memory_space=pltpu.VMEM),
            scratch_shapes=[
                pltpu.VMEM((2, side, b // 2, hl, k), bf),
                pltpu.VMEM((nc, 2 * side, nb, tile, k), bf),
                pltpu.VMEM((NBUF, t, k), bf),
                pltpu.VMEM((NSLOT, nb, half, lorav + LANES), f32),
                pltpu.VMEM((NSLOT, nb, half, lorav + LANES), f32),
                pltpu.VMEM((nc, nb, half, lorav + LANES), f32),
                pltpu.VMEM((nc, side, nb, tile, lorav), bf),
                pltpu.VMEM((nc, 2, nb // 2, tile, lorav), bf),
                pltpu.VMEM((nc, side, nb, tile, lorav), bf),
                pltpu.VMEM((2, nc // 2, nb, LANES), f32),
                pltpu.VMEM((2, side, nc // 2, nb, LANES), f32),
                pltpu.VMEM((nc, side, nb, hl, lorav), f32),
                pltpu.VMEM((nc, 2, nb // 2, hl, lorav), f32),
                pltpu.VMEM((nc, side, nb, hl, lorav), f32),
                pltpu.VMEM((2, nc // 2, nb, LANES), f32),
                pltpu.VMEM((2, side, nc // 2, nb, LANES), f32),
                pltpu.VMEM((side, nb, LANES), f32),
                pltpu.VMEM((2 * half, t), f32), pltpu.VMEM((2 * half, t), f32),
                dma((NBUF,)),
                dma((2, 2, 4)), dma((2, 2, 4)), dma((nc, 4)), dma((nc, 4)),
                dma((nc, side)), dma((nc, side)),
                dma((nc,)), dma((nc,)),
                dma((nc, 6)), dma((nc, 6)), dma((2, nc // 4, side - 1)), dma((2, nc // 4, side - 1)),
                dma((nc, 6)), dma((nc, 6)), dma((2, nc // 4, side - 1)), dma((2, nc // 4, side - 1)),
            ],
            compiler_params=pltpu.CompilerParams(collective_id=0, has_side_effects=True,
                                                 vmem_limit_bytes=63 * 1024 * 1024),
        )(q, cache.reshape(b, t, k), lens)

    return jax.shard_map(local, mesh=mesh, in_specs=(P('dp', 'dcp', None), P('dp', None, 'dcp', None, None), P('dp')),
                         out_specs=P('dp', 'dcp', None), check_vma=False)
```

```python
import functools
import math

import jax
import jax.numpy as jnp
from jax import lax
from jax.experimental import pallas as pl
from jax.experimental.pallas import tpu as pltpu
from jax.sharding import PartitionSpec as P

ROPE = 64
QK_DIM = 192
SCALE = QK_DIM ** -0.5
NEG = float('-inf')
LANES = 128
NBUF = 8
NSLOT = 4
LAG = 2


def mod(a, b):
    return a % b if isinstance(a, int) else lax.rem(a, b)


def div(a, b):
    return a // b if isinstance(a, int) else lax.div(a, b)


def kernel(n, side, nc, nb, page, q_hbm, cache_ref, lens_ref, out_ref,
           q_ref, g1, qall, cbuf, own, osend, orecv, p1s, p1x, p1r, l1s, l1r, p2s, p2x, p2r, l2s, l2r, wrow, sb0, sb1,
           csem, a1s, a1r, a2s, a2r, a3s, a3r, ods, odr, s1, r1, sl1, rr1, s2, r2, sl2, rr2):
    hl = q_ref.shape[1]
    k = q_ref.shape[2]
    t = cbuf.shape[1]
    lorav = k - ROPE
    tile = side * hl
    half = side * tile
    total = nc * nb
    each_type = total // 2

    def row(c):
        return (div(c, 2)) * nb

    def seq(b):
        c = div(b, nb)
        return (mod(c, 2)) * each_type + row(c) + mod(b, nb)

    me = lax.axis_index('dcp')
    core = me % 2
    x = (me // 2) % side
    y = me // (2 * side)
    dists = tuple(range(1, side))

    def at(yy, xx, cc):
        return {'dcp': (yy * side + xx) * 2 + cc}

    sib = at(y, x, 1 - core)

    xs = [(x + d) % side for d in range(side)]
    ys = [(y + d) % side for d in range(side)]
    xid = [(y * side + v) * 2 + core for v in xs]
    yid = [(v * side + x) * 2 + core for v in ys]

    def pos_at(c, axis, d):
        odd = mod(c, 2) if axis == 0 else 1 - mod(c, 2)
        return xs[d] + odd * (ys[d] - xs[d])

    def axes(c):
        def along(axis):
            odd = mod(c, 2) if axis == 0 else 1 - mod(c, 2)
            return pos_at(c, axis, 0), lambda d: {'dcp': xid[d] + odd * (yid[d] - xid[d])}

        return along(0), along(1)

    def rcopy(src, dst, ss, rs, dev):
        return pltpu.make_async_remote_copy(src_ref=src, dst_ref=dst, send_sem=ss, recv_sem=rs, device_id=dev,
                                            device_id_type=pl.DeviceIdType.MESH)

    hb = nb // 2

    def part(h):
        return pl.ds(h * hb, hb)

    near = (1, side - 1)

    bounds = [0, min(2 * nb, each_type), each_type]
    pieces = [p for p in range(len(bounds) - 1) if bounds[p + 1] > bounds[p]]

    def ag1(p, ty, h):
        (m1, peer), _ = axes(ty)
        at_ = pl.ds(bounds[p], bounds[p + 1] - bounds[p])
        return rcopy(q_ref.at[pl.ds(ty * each_type + bounds[p], bounds[p + 1] - bounds[p])], g1.at[ty, m1, at_],
                     a1s.at[p, ty, h], a1r.at[p, ty, h], peer(near[h]))

    def ag1f(p, ty, h):
        (m1, peer), _ = axes(ty)
        a = (m1 + side - near[h]) % side
        size = (bounds[p + 1] - bounds[p]) // 2
        at_ = pl.ds(bounds[p] + h * size, size)
        return rcopy(g1.at[ty, a, at_], g1.at[ty, a, at_], a1s.at[p, ty, 2 + h], a1r.at[p, ty, 2 + h], peer(near[h]))

    def ag2(c, h):
        _, (m2, peer) = axes(c)
        return rcopy(qall.at[c, m2], qall.at[c, m2], a2s.at[c, h], a2r.at[c, h], peer(near[h]))

    def ag2f(c, h):
        _, (_, peer) = axes(c)
        a = pos_at(c, 1, near[1 - h])
        return rcopy(qall.at[c, a, part(h)], qall.at[c, a, part(h)], a2s.at[c, 2 + h], a2r.at[c, 2 + h], peer(near[h]))

    def ag3(c, d):
        a = pos_at(c, 1, (side - d) % side)
        return rcopy(qall.at[c, a], qall.at[c, side + a], a3s.at[c, d], a3r.at[c, d], sib)

    def od(c):
        return rcopy(osend.at[mod(c, NSLOT)], orecv.at[c], ods.at[c], odr.at[c], sib)

    def rs1(c, h):
        _, (m2, peer) = axes(c)
        return rcopy(p1s.at[c, pos_at(c, 1, near[h])], p1r.at[c, m2], s1.at[c, h], r1.at[c, h], peer(near[h]))

    def rs1x(c, h):
        _, (m2, peer) = axes(c)
        return rcopy(p1s.at[c, pos_at(c, 1, 2), part(h)], p1x.at[c, h], s1.at[c, 2 + h], r1.at[c, 2 + h], peer(near[h]))

    def rs1f(c, h):
        _, (m2, peer) = axes(c)
        a = pos_at(c, 1, near[1 - h])
        return rcopy(p1x.at[c, h], p1r.at[c, a, part(h)], s1.at[c, 4 + h], r1.at[c, 4 + h], peer(near[h]))

    def both(c):
        return pl.ds((div(c, 4)) * 2, 2)

    def rl1(c, d):
        _, (m2, peer) = axes(c)
        return rcopy(l1s.at[mod(c, 2), both(c)], l1r.at[mod(c, 2), m2, both(c)], sl1.at[mod(c, 2), div(c, 4), d - 1],
                     rr1.at[mod(c, 2), div(c, 4), d - 1], peer(d))

    def rs2(c, h):
        (m1, peer), _ = axes(c)
        return rcopy(p2s.at[c, pos_at(c, 0, near[h])], p2r.at[c, m1], s2.at[c, h], r2.at[c, h], peer(near[h]))

    def rs2x(c, h):
        (m1, peer), _ = axes(c)
        return rcopy(p2s.at[c, pos_at(c, 0, 2), part(h)], p2x.at[c, h], s2.at[c, 2 + h], r2.at[c, 2 + h], peer(near[h]))

    def rs2f(c, h):
        (m1, peer), _ = axes(c)
        a = pos_at(c, 0, near[1 - h])
        return rcopy(p2x.at[c, h], p2r.at[c, a, part(h)], s2.at[c, 4 + h], r2.at[c, 4 + h], peer(near[h]))

    def rl2(c, d):
        (m1, peer), _ = axes(c)
        return rcopy(l2s.at[mod(c, 2), both(c)], l2r.at[mod(c, 2), m1, both(c)], sl2.at[mod(c, 2), div(c, 4), d - 1],
                     rr2.at[mod(c, 2), div(c, 4), d - 1], peer(d))

    def cload(b):
        return pltpu.make_async_copy(cache_ref.at[seq(b)], cbuf.at[mod(b, NBUF)], csem.at[mod(b, NBUF)])

    q_copy = pltpu.make_async_copy(q_hbm, q_ref, csem.at[NBUF])
    q_copy.start()
    for b in range(min(NBUF, total)):
        cload(b).start()

    barrier = pltpu.get_barrier_semaphore()
    peers = [sib] + [at(y, (x + d) % side, core) for d in dists] + [at((y + d) % side, x, core) for d in dists]
    for dev in peers:
        pl.semaphore_signal(barrier, inc=1, device_id=dev, device_id_type=pl.DeviceIdType.MESH)
    pl.semaphore_wait(barrier, len(peers))
    q_copy.wait()

    def gather_far_rows(p):
        for ty in range(2):
            for h in range(2):
                ag1f(p, ty, h).wait_recv()

    for p in pieces:
        for ty in range(2):
            for h in range(2):
                ag1(p, ty, h).start()
    for p in pieces:
        for ty in range(2):
            (m1, _), _ = axes(ty)
            g1[ty, m1, bounds[p]:bounds[p + 1]] = q_ref[ty * each_type + bounds[p]:ty * each_type + bounds[p + 1]]
            for h in range(2):
                ag1(p, ty, h).wait_recv()
                ag1f(p, ty, h).start()
    gather_far_rows(0)

    def gather_first(c):
        _, (m2, _) = axes(c)
        if len(pieces) > 1:
            @pl.when(c == 2 * bounds[1] // nb)
            def _():
                gather_far_rows(1)

        def body(i, _):
            parts = [g1[mod(c, 2), a, row(c) + i].astype(jnp.float32) for a in range(side)]
            qall[c, m2, i] = jnp.concatenate(parts, axis=0).astype(qall.dtype)
            return 0

        lax.fori_loop(0, nb, body, 0)
        for h in range(2):
            ag2(c, h).start()
        ag3(c, 0).start()

    def gather_second(c):
        for h in range(2):
            ag2(c, h).wait_recv()
            ag2f(c, h).start()
            ag3(c, near[h]).start()

    def gather_far(c):
        for h in range(2):
            ag2f(c, h).wait_recv()
        ag3(c, 2).start()

    def gather_third(c):
        for d in range(side):
            ag3(c, d).wait_recv()

    tpos = lax.broadcasted_iota(jnp.int32, (1, t), 1)
    pos = (tpos // page) * (page * n) + me * page + tpos % page

    def scores(b, ref):
        ref[...] = lax.dot_general(qall[div(b, nb), :, mod(b, nb)].reshape(2 * half, k), cbuf[mod(b, NBUF)],
                                   (((1,), (1,)), ((), ())), preferred_element_type=jnp.float32)

    def attend(c, i, ref):
        b = c * nb + i
        s = jnp.where(pos < lens_ref[seq(b)], ref[...], NEG)
        m = jnp.max(s, axis=1, keepdims=True)
        ms = jnp.where(m == NEG, 0.0, m)
        p = jnp.exp((s - ms) * SCALE)
        l = jnp.sum(p, axis=1, keepdims=True)
        acc = lax.dot_general(p.astype(jnp.bfloat16), cbuf[mod(b, NBUF), :, :lorav], (((1,), (0,)), ((), ())),
                              preferred_element_type=jnp.float32)
        ls = jnp.where(l > 0.0, l, 1.0)
        o = acc * (1.0 / ls)
        lse = jnp.broadcast_to(jnp.where(l > 0.0, ms * SCALE + jnp.log(ls), NEG), (2 * half, LANES))
        own[mod(c, NSLOT), i, :, :lorav] = o[:half]
        own[mod(c, NSLOT), i, :, lorav:] = lse[:half]
        osend[mod(c, NSLOT), i, :, :lorav] = o[half:]
        osend[mod(c, NSLOT), i, :, lorav:] = lse[half:]

    diag = lax.broadcasted_iota(jnp.int32, (half, LANES), 0) == lax.broadcasted_iota(jnp.int32, (half, LANES), 1)

    def pair_one(c, i):
        la = own[mod(c, NSLOT), i, :, lorav:]
        lb = orecv[c, i, :, lorav:]
        top = jnp.maximum(la, lb)
        ts = jnp.where(top == NEG, 0.0, top)
        wa = jnp.exp(la - ts)
        wb = jnp.exp(lb - ts)
        ws = wa + wb
        wss = jnp.where(ws > 0.0, ws, 1.0)
        inv = 1.0 / wss
        wa = wa * inv
        wb = wb * inv
        for j in range(lorav // LANES):
            cols = slice(j * LANES, (j + 1) * LANES)
            v = (wa * own[mod(c, NSLOT), i, :, cols] + wb * orecv[c, i, :, cols]).astype(jnp.bfloat16)
            p1s[c, :, i, :, cols] = v.reshape(side, tile, LANES)
        lse = jnp.where(ws > 0.0, ts + jnp.log(wss), NEG)
        l1s[mod(c, 2), div(c, 2), pl.ds(i, 1)] = jnp.sum(jnp.where(diag, lse, 0.0), axis=0, keepdims=True)

    def compute(c):
        @pl.when(c >= NSLOT)
        def _():
            od(jnp.maximum(c - NSLOT, 0)).wait_send()

        @pl.when(c == 0)
        def _():
            cload(0).wait()
            scores(0, sb0)

        def two(j, merged):
            b = c * nb + 2 * j
            cload(b + 1).wait()

            @pl.when(b + 2 < total)
            def _():
                cload(b + 2).wait()

            scores(b + 1, sb1)
            if merged:
                pair_one(jnp.maximum(c - LAG, 0), 2 * j)
                pair_one(jnp.maximum(c - LAG, 0), 2 * j + 1)
            attend(c, 2 * j, sb0)
            scores(jnp.minimum(b + 2, total - 1), sb0)
            attend(c, 2 * j + 1, sb1)
            for later in range(NBUF, NBUF + 2):
                @pl.when(b + later < total)
                def _():
                    cload(b + later).start()

            return 0

        @pl.when(c < LAG)
        def _():
            lax.fori_loop(0, nb // 2, lambda j, _: two(j, False), 0)

        @pl.when(c >= LAG)
        def _():
            od(jnp.maximum(c - LAG, 0)).wait_recv()
            lax.fori_loop(0, nb // 2, lambda j, _: two(j, True), 0)

        od(c).start()

    def pair(c):
        @pl.when(c >= nc - LAG)
        def _():
            od(c).wait_recv()

            def one(i, _):
                pair_one(c, i)
                return 0

            lax.fori_loop(0, nb, one, 0)

        for h in range(2):
            rs1x(c, h).start()

        @pl.when(mod(div(c, 2), 2) == 1)
        def _():
            for d in dists:
                rl1(c, d).start()

        for h in range(2):
            rs1(c, h).start()

    def pair_relay(c):
        for h in range(2):
            rs1x(c, h).wait_recv()
            rs1f(c, h).start()

    def weights(ls):
        top = functools.reduce(jnp.maximum, ls)
        ts = jnp.where(top == NEG, 0.0, top)
        w = [jnp.exp(v - ts) for v in ls]
        ws = functools.reduce(jnp.add, w)
        wss = jnp.where(ws > 0.0, ws, 1.0)
        inv = 1.0 / wss
        for j, v in enumerate(w):
            wrow[j] = v * inv
        return jnp.where(ws > 0.0, ts + jnp.log(wss), NEG)

    def combine(i, rows, first, srcs):
        sel = (lax.broadcasted_iota(jnp.int32, (rows, LANES), 0) + first
               == lax.broadcasted_iota(jnp.int32, (rows, LANES), 1))
        tot = None
        for j, src in enumerate(srcs):
            w = jnp.broadcast_to(wrow[j, pl.ds(i, 1)], (rows, LANES))
            w = jnp.sum(jnp.where(sel, w, 0.0), axis=1, keepdims=True)
            term = w * src[i].astype(jnp.float32)
            tot = term if tot is None else tot + term
        return tot

    def second(c):
        (m1, _), (m2, _) = axes(c)
        for h in range(2):
            rs1(c, h).wait_recv()
            rs1f(c, h).wait_recv()

        @pl.when(mod(div(c, 2), 2) == 0)
        def _():
            for d in dists:
                rl1(c, d).wait_recv()

        idx = [pos_at(c, 1, d) for d in dists]
        l2s[mod(c, 2), div(c, 2)] = weights([l1s[mod(c, 2), div(c, 2)]] + [l1r[mod(c, 2), a, div(c, 2)] for a in idx])
        srcs = [p1s.at[c, m2]] + [p1r.at[c, a] for a in idx]

        def one(i, _):
            v = combine(i, tile, m2 * tile, srcs)
            for a in range(side):
                p2s[c, a, i] = v[a * hl:(a + 1) * hl]
            return 0

        lax.fori_loop(0, nb, one, 0)
        for h in range(2):
            rs2x(c, h).start()

        @pl.when(mod(div(c, 2), 2) == 1)
        def _():
            for d in dists:
                rl2(c, d).start()

        for h in range(2):
            rs2(c, h).start()

    def second_relay(c):
        for h in range(2):
            rs2x(c, h).wait_recv()
            rs2f(c, h).start()

    def final(c):
        (m1, _), (m2, _) = axes(c)
        for h in range(2):
            rs2(c, h).wait_recv()
            rs2f(c, h).wait_recv()

        @pl.when(mod(div(c, 2), 2) == 0)
        def _():
            for d in dists:
                rl2(c, d).wait_recv()

        idx = [pos_at(c, 0, d) for d in dists]
        weights([l2s[mod(c, 2), div(c, 2)]] + [l2r[mod(c, 2), a, div(c, 2)] for a in idx])
        srcs = [p2s.at[c, m1]] + [p2r.at[c, a] for a in idx]

        def one(i, _):
            out_ref[seq(c * nb + i)] = combine(i, hl, m2 * tile + m1 * hl, srcs).astype(out_ref.dtype)
            return 0

        lax.fori_loop(0, nb, one, 0)

    def each(stage):
        def one(c, _):
            stage(c)
            return 0

        lax.fori_loop(0, nc, one, 0)

    stages = ((gather_third, 12), (compute, 13), (pair, 15), (gather_first, 0), (pair_relay, 18), (gather_second, 5),
              (gather_far, 9), (second, 23), (second_relay, 31), (final, 40))

    def step(i, _):
        for stage, delay in stages:
            @pl.when((i >= delay) & (i < delay + nc))
            def _():
                stage(jnp.maximum(i - delay, 0))

        return 0

    lax.fori_loop(0, nc + max(d for _, d in stages), step, 0)

    def drain(c):
        for h in range(2):
            for cp in (ag2, ag2f, rs1, rs1x, rs1f, rs2, rs2x, rs2f):
                cp(c, h).wait_send()

        @pl.when(mod(div(c, 2), 2) == 1)
        def _():
            for d in dists:
                rl1(c, d).wait_send()
                rl2(c, d).wait_send()

        for d in range(side):
            ag3(c, d).wait_send()

        @pl.when(c >= nc - NSLOT)
        def _():
            od(c).wait_send()

    each(drain)
    for p in pieces:
        for ty in range(2):
            for h in range(2):
                ag1(p, ty, h).wait_send()
                ag1f(p, ty, h).wait_send()


def solution(mesh):
    n = mesh.shape['dcp']
    side = math.isqrt(n // 2)

    def local(q, cache, lens):
        b, hl, k = q.shape
        t = cache.shape[1] * cache.shape[3]
        lorav = k - ROPE
        nb = min(4, max(1, b // 4))
        nc = div(b, nb)
        tile = side * hl
        half = side * tile
        bf, f32 = jnp.bfloat16, jnp.float32
        dma = pltpu.SemaphoreType.DMA
        return pl.pallas_call(
            functools.partial(kernel, n, side, nc, nb, cache.shape[3]),
            out_shape=jax.ShapeDtypeStruct((b, hl, lorav), bf),
            in_specs=[pl.BlockSpec(memory_space=pl.ANY), pl.BlockSpec(memory_space=pl.ANY),
                      pl.BlockSpec(memory_space=pltpu.SMEM)],
            out_specs=pl.BlockSpec(memory_space=pltpu.VMEM),
            scratch_shapes=[
                pltpu.VMEM((b, hl, k), bf),
                pltpu.VMEM((2, side, b // 2, hl, k), bf),
                pltpu.VMEM((nc, 2 * side, nb, tile, k), bf),
                pltpu.VMEM((NBUF, t, k), bf),
                pltpu.VMEM((NSLOT, nb, half, lorav + LANES), f32),
                pltpu.VMEM((NSLOT, nb, half, lorav + LANES), f32),
                pltpu.VMEM((nc, nb, half, lorav + LANES), f32),
                pltpu.VMEM((nc, side, nb, tile, lorav), bf),
                pltpu.VMEM((nc, 2, nb // 2, tile, lorav), bf),
                pltpu.VMEM((nc, side, nb, tile, lorav), bf),
                pltpu.VMEM((2, nc // 2, nb, LANES), f32),
                pltpu.VMEM((2, side, nc // 2, nb, LANES), f32),
                pltpu.VMEM((nc, side, nb, hl, lorav), f32),
                pltpu.VMEM((nc, 2, nb // 2, hl, lorav), f32),
                pltpu.VMEM((nc, side, nb, hl, lorav), f32),
                pltpu.VMEM((2, nc // 2, nb, LANES), f32),
                pltpu.VMEM((2, side, nc // 2, nb, LANES), f32),
                pltpu.VMEM((side, nb, LANES), f32),
                pltpu.VMEM((2 * half, t), f32), pltpu.VMEM((2 * half, t), f32),
                dma((NBUF + 1,)),
                dma((2, 2, 4)), dma((2, 2, 4)), dma((nc, 4)), dma((nc, 4)),
                dma((nc, side)), dma((nc, side)),
                dma((nc,)), dma((nc,)),
                dma((nc, 6)), dma((nc, 6)), dma((2, nc // 4, side - 1)), dma((2, nc // 4, side - 1)),
                dma((nc, 6)), dma((nc, 6)), dma((2, nc // 4, side - 1)), dma((2, nc // 4, side - 1)),
            ],
            compiler_params=pltpu.CompilerParams(collective_id=0, has_side_effects=True,
                                                 vmem_limit_bytes=63 * 1024 * 1024),
        )(q, cache.reshape(b, t, k), lens)

    return jax.shard_map(local, mesh=mesh, in_specs=(P('dp', 'dcp', None), P('dp', None, 'dcp', None, None), P('dp')),
                         out_specs=P('dp', 'dcp', None), check_vma=False)
```
